256 devices in a mesh: blk: 128 (over z, x, y), rep: 2 (over core).
Axes of the slice: x: 4, y: 4, z: 8, core: 2. Of those that a mesh axis runs over, the one named last changes fastest.
Arguments:
- points: float32 [128, 3, 8192], P('blk'), may hold values from -6 to 6
- normals: float32 [128, 3, 8192], P('blk'), may hold values from -6 to 6
- src_block: int32 [8, 128, 1, 16], P(None, 'blk', None, 'rep'), may hold values from 0 to 63
- tgt_index: int32 [8, 128, 1, 16, 128], P(None, 'blk', None, 'rep'), may hold values from 0 to 8191
- active: int32 [8, 128, 1], P(None, 'blk'), may hold values from 0 to 16
Outputs:
- diag_hess: float32 [128, 36], P('blk')
- gradient: float32 [128, 6], P('blk')
- pair_hess: float32 [8, 128, 1, 36], P(None, 'blk')
The draws below stay inside these ranges and needn't reach their ends.
Inputs may be any that keep to these rules, and one draw needn't show every extreme that they name: Slots j with j >= active contribute nothing.
All inputs are finite; a program needn't handle non-finite values.
Results may differ from the reference program's by a relative error of at most 0.00017.
Values sent between devices are 32-bit elements; how exact they have to be, the bound alone decides.
No kernel may reach another device: no remote copies, remote signals or barrier semaphores. Data moves between devices by JAX's collectives and lax.ppermute only.
A program may use at most 64 MiB of HBM per device.

```python
import jax
import jax.numpy as jnp
from jax import lax

SC = 1
P_SIZE = 8192
NB = 16
BLOCK = 128
ROUNDS = 8
NSCANS = 128
N_BLK = 128


def place_ends(values, key, low, high):
    longest = values.shape.index(max(values.shape))
    spots = []
    for shift in (0, 1):
        where = [jax.random.randint(jax.random.fold_in(key, axis), (), 0, length) for axis, length in enumerate(values.shape)]
        where[longest] = (where[longest] + shift) % values.shape[longest]
        spots.append(tuple(where))
    return values.at[spots[0]].set(low).at[spots[1]].set(high)


def level_of(rng, extent, shards, low, high):
    level = 1.0
    for dim, shards_of in shards:
        steps = jax.random.uniform(jax.random.fold_in(jax.random.fold_in(rng, 6), dim), (shards_of,), jnp.float32, low / len(shards), high / len(shards))
        level = level * jnp.repeat(jnp.exp(steps), extent[dim] // shards_of).reshape((-1,) + (1,) * (len(extent) - 1 - dim))
    return level


def gaussian(key, extent, width, limit, pieces=(), kind=jnp.bfloat16):
    gain = level_of(key, extent, pieces, -0.22, 0.18) if pieces else 1.0
    drawn = jax.random.normal(key, extent, jnp.float32) * width * gain
    return jnp.minimum(jnp.maximum(drawn, -limit), limit).astype(kind)


def setup_inputs(seed: int = 0) -> dict:
    key_of = jax.random.split(jax.random.key(seed), 6)
    return {
        "points": gaussian(key_of[0], (NSCANS, 3, P_SIZE), 0.5, 6.0, ((0, 128),), jnp.float32),
        "normals": gaussian(key_of[1], (NSCANS, 3, P_SIZE), 1.0, 6.0, ((0, 128),), jnp.float32),
        "src_block": place_ends(jax.random.randint(key_of[2], (ROUNDS, NSCANS, SC, NB), 0, P_SIZE // BLOCK), jax.random.fold_in(key_of[2], 1), 0, (P_SIZE // BLOCK) - 1).astype(jnp.int32),
        "tgt_index": place_ends(jax.random.randint(key_of[3], (ROUNDS, NSCANS, SC, NB, BLOCK), 0, P_SIZE), jax.random.fold_in(key_of[3], 1), 0, P_SIZE - 1).astype(jnp.int32),
        "active": place_ends(jax.random.randint(key_of[4], (ROUNDS, NSCANS, SC), 0, NB + 1), jax.random.fold_in(key_of[4], 1), 0, NB).astype(jnp.int32),
    }


def reference(points, normals, src_block, tgt_index, active):
    nscans = points.shape[0]
    npts = points.shape[2]
    slots = NB * BLOCK
    flat_p = jnp.moveaxis(points, 1, 0).reshape(3, -1)
    flat_n = jnp.moveaxis(normals, 1, 0).reshape(3, -1)
    lanes = jnp.arange(BLOCK, dtype=jnp.int32)
    owner = jnp.arange(nscans, dtype=jnp.int32) // SC
    local = jnp.arange(SC, dtype=jnp.int32)
    scans = jnp.arange(nscans, dtype=jnp.int32)
    slot_block = jnp.arange(slots, dtype=jnp.int32) // BLOCK
    diag = jnp.zeros((nscans, 36), jnp.float32)
    grad = jnp.zeros((nscans, 6), jnp.float32)
    pairs = []
    for k in range(1, ROUNDS + 1):
        tscan = (((owner[:, None] - k) % N_BLK) * SC + local[None, :]).astype(jnp.int32)
        sidx = (scans[:, None, None, None] * npts + src_block[k - 1][:, :, :, None] * BLOCK + lanes).reshape(nscans, SC, slots)
        tidx = tscan[:, :, None] * npts + tgt_index[k - 1].reshape(nscans, SC, slots)
        p = flat_p[:, sidx]
        q = flat_p[:, tidx]
        n = flat_n[:, tidx]
        live = (slot_block[None, None, :] < active[k - 1][:, :, None]).astype(jnp.float32)
        resid = jnp.sum(n * (p - q), axis=0)
        weight = live / (1.0 + resid * resid)
        jacob = jnp.stack([p[1] * n[2] - p[2] * n[1], p[2] * n[0] - p[0] * n[2], p[0] * n[1] - p[1] * n[0], n[0], n[1], n[2]])
        gram = jnp.einsum('iast,jast->asij', jacob * weight, jacob, precision=lax.Precision.HIGHEST) / (NB * BLOCK)
        push = jnp.einsum('iast,ast->asi', jacob, weight * resid, precision=lax.Precision.HIGHEST) / (NB * BLOCK)
        gram = gram.reshape(nscans, SC, 36)
        pairs.append(gram)
        diag = diag + gram.sum(1)
        grad = grad + push.sum(1)
        diag = diag.at[tscan.reshape(-1)].add(gram.reshape(-1, 36))
        grad = grad.at[tscan.reshape(-1)].add(-push.reshape(-1, 6))
    scale = 2.0 * ROUNDS * SC
    return diag / scale, grad / scale, jnp.stack(pairs)
```

```python
import functools

import jax
import jax.numpy as jnp
from jax import lax
from jax.experimental import pallas as pl
from jax.experimental.pallas import tpu as pltpu
from jax.sharding import PartitionSpec as P

NB = 16
BLOCK = 128
LANES = 128
SUBLANES = 8


def routed(block, blk, shifts, cross):
    route = []
    for i in range(blk):
        for r in range(2):
            target = (i + shifts[r]) % blk
            route.append((i * 2 + r, target * 2 + (1 - r if cross else r)))
    return lax.ppermute(block, ("blk", "rep"), route)


def pick_lanes(row, lanes):
    return lax.gather(
        row,
        lanes[:, :, None],
        lax.GatherDimensionNumbers(
            offset_dims=(),
            collapsed_slice_dims=(1,),
            start_index_map=(1,),
            operand_batching_dims=(0,),
            start_indices_batching_dims=(0,),
        ),
        slice_sizes=(1, 1),
        mode=lax.GatherScatterMode.PROMISE_IN_BOUNDS,
    )


def pack_kernel(src_ref, active_ref, points_ref, index_ref, *outs):
    half = lax.axis_index("rep")
    slot = lax.broadcasted_iota(jnp.int32, (SUBLANES, LANES), 0) + half * SUBLANES
    for i, out in enumerate(outs):
        m, cross = i // 2, i % 2
        k = 2 * m + half if cross else 2 * m + 1 - half
        for j in range(SUBLANES):
            b = src_ref[k, j]
            for c in range(3):
                out[c, pl.ds(j, 1), :] = points_ref[c, pl.ds(b, 1), :]
        live = slot < active_ref[0, k]
        out[3] = jnp.where(live, index_ref[k], -1).astype(jnp.float32)


def pair_kernel(points_ref, normals_ref, *refs):
    messages, rows, total_ref = refs[:8], refs[8:12], refs[12]
    index_s, picked_s, sums_s = refs[13:]
    for i in range(8):
        index_s[i] = messages[i][3].astype(jnp.int32)

    def gather(i, carry):
        index = index_s[i]
        lanes = index & (LANES - 1)
        high = index >> 7
        found = [jnp.zeros((SUBLANES, LANES), jnp.float32) for _ in range(6)]
        for r in range(points_ref.shape[1]):
            here = high == r
            for c in range(6):
                table = points_ref if c < 3 else normals_ref
                row = jnp.broadcast_to(table[c % 3, pl.ds(r, 1), :], (SUBLANES, LANES))
                found[c] = jnp.where(here, pick_lanes(row, lanes), found[c])
        for c in range(6):
            picked_s[i, c] = found[c]
        return carry

    lax.fori_loop(0, 8, gather, 0)
    for m in range(4):
        parts = []
        for i in (2 * m, 2 * m + 1):
            p = [messages[i][c] for c in range(3)]
            q = [picked_s[i, c] for c in range(3)]
            n = [picked_s[i, 3 + c] for c in range(3)]
            resid = n[0] * (p[0] - q[0]) + n[1] * (p[1] - q[1]) + n[2] * (p[2] - q[2])
            weight = 1.0 / (1.0 + resid * resid)
            jacob = [
                p[1] * n[2] - p[2] * n[1],
                p[2] * n[0] - p[0] * n[2],
                p[0] * n[1] - p[1] * n[0],
                n[0],
                n[1],
                n[2],
            ]
            scaled = [weight * x for x in jacob]
            terms = [scaled[a] * jacob[b] for a in range(6) for b in range(a, 6)]
            terms += [scaled[a] * resid for a in range(6)]
            parts.append(terms)
        for t in range(27):
            sums_s[pl.ds(4 * t + m, 1), :] = jnp.sum(parts[0][t] + parts[1][t], axis=0, keepdims=True)

    row = lax.broadcasted_iota(jnp.int32, (SUBLANES, LANES), 0)
    lane = lax.broadcasted_iota(jnp.int32, (SUBLANES, LANES), 1)
    odd = row // 4
    first, second = lane // 6, lane % 6
    low, high = jnp.minimum(first, second), jnp.maximum(first, second)
    gram_term = jnp.where(lane < 36, low * (11 - low) // 2 + high, -1)
    push_term = jnp.where(lane < 6, 21 + lane, -1)
    gram = jnp.zeros((SUBLANES, LANES), jnp.float32)
    push = jnp.zeros((SUBLANES, LANES), jnp.float32)
    for g in range(14):
        size = 8 if g < 13 else 4
        column = jnp.sum(sums_s[pl.ds(8 * g, 8), :], axis=1, keepdims=True)
        term = 2 * g + odd
        if 2 * g < 21:
            gram = jnp.where(gram_term == term, column, gram)
        if 2 * g + 1 >= 21:
            push = jnp.where(push_term == term, column, push)
    scale = 1.0 / (NB * BLOCK)
    gram = (gram[:4] + gram[4:]) * scale
    push = (push[:4] + push[4:]) * scale
    for m in range(4):
        rows[m][0:1, :] = gram[m : m + 1]
        rows[m][1:2, :] = push[m : m + 1]
    total_ref[0:1, :] = jnp.sum(gram, axis=0, keepdims=True)
    total_ref[1:2, :] = -jnp.sum(push, axis=0, keepdims=True)


def finish_kernel(*refs, scale):
    rows, totals, (diag_ref, grad_ref, pair_ref) = refs[:8], refs[8:10], refs[10:]
    half = lax.axis_index("rep")
    total = totals[0][...] + totals[1][...]
    for i in range(8):
        m, cross = i // 2, i % 2
        k = 2 * m + half if cross else 2 * m + 1 - half
        got = rows[i][...]
        pair_ref[pl.ds(k, 1), :] = got[0:1, :36]
        total = total + got
    diag_ref[...] = total[0:1, :36] * scale
    grad_ref[...] = total[1:2, :6] * scale


def body(points, normals, src_block, tgt_index, active, *, blk):
    rounds = src_block.shape[0]
    table = (3, points.shape[2] // LANES, LANES)
    points = points.reshape(table)
    normals = normals.reshape(table)
    vmem = pl.BlockSpec(memory_space=pltpu.VMEM)
    smem = pl.BlockSpec(memory_space=pltpu.SMEM)
    f32 = jnp.float32
    messages = pl.pallas_call(
        pack_kernel,
        in_specs=[smem, smem, vmem, vmem],
        out_specs=[vmem] * 8,
        out_shape=[jax.ShapeDtypeStruct((4, SUBLANES, LANES), f32)] * 8,
        name="pack",
    )(src_block.reshape(rounds, -1), active.reshape(1, rounds), points, tgt_index.reshape(rounds, SUBLANES, BLOCK))
    offsets = [(2 * m + 2, 2 * m + 1) for m in range(4)]
    there = []
    for i in range(8):
        even, odd = offsets[i // 2]
        cross = i % 2 == 1
        there.append(routed(messages[i], blk, (-odd, -even) if cross else (-even, -odd), cross))
    *rows, total = pl.pallas_call(
        pair_kernel,
        in_specs=[vmem] * 10,
        out_specs=[vmem] * 5,
        out_shape=[jax.ShapeDtypeStruct((2, LANES), f32)] * 5,
        scratch_shapes=[
            pltpu.VMEM((8, SUBLANES, LANES), jnp.int32),
            pltpu.VMEM((8, 6, SUBLANES, LANES), f32),
            pltpu.VMEM((112, LANES), f32),
        ],
        name="pairs",
    )(points, normals, *there)
    back = []
    for i in range(8):
        even, odd = offsets[i // 2]
        back.append(routed(rows[i // 2], blk, (even, odd), i % 2 == 1))
    other = routed(total, blk, (0, 0), True)
    diag, grad, pairs = pl.pallas_call(
        functools.partial(finish_kernel, scale=1.0 / (2.0 * rounds)),
        in_specs=[vmem] * 10,
        out_specs=[vmem] * 3,
        out_shape=[
            jax.ShapeDtypeStruct((1, 36), f32),
            jax.ShapeDtypeStruct((1, 6), f32),
            jax.ShapeDtypeStruct((rounds, 36), f32),
        ],
        name="finish",
    )(*back, total, other)
    return diag, grad, pairs.reshape(rounds, 1, 1, 36)


def solution(mesh):
    return jax.shard_map(
        functools.partial(body, blk=mesh.shape["blk"]),
        mesh=mesh,
        in_specs=(
            P("blk", None, None),
            P("blk", None, None),
            P(None, "blk", None, "rep"),
            P(None, "blk", None, "rep", None),
            P(None, "blk", None),
        ),
        out_specs=(P("blk", None), P("blk", None), P(None, "blk", None, None)),
        check_vma=False,
    )
```

```python
import functools

import jax
import jax.numpy as jnp
from jax import lax
from jax.experimental import pallas as pl
from jax.experimental.pallas import tpu as pltpu
from jax.sharding import PartitionSpec as P

NB = 16
BLOCK = 128
LANES = 128
SUBLANES = 8


VMEM = pl.BlockSpec(memory_space=pltpu.VMEM)
SMEM = pl.BlockSpec(memory_space=pltpu.SMEM)


def routed(block, blk, shifts):
    route = [(i * 2 + r, (i + shifts[r]) % blk * 2 + r) for i in range(blk) for r in range(2)]
    return lax.ppermute(block, ("blk", "rep"), route)


def swapped(block):
    return lax.ppermute(block, "rep", [(0, 1), (1, 0)])


def near(x):
    return pltpu.with_memory_space_constraint(x, pltpu.VMEM)


def pick_lanes(row, lanes):
    return lax.gather(
        row,
        lanes[:, :, None],
        lax.GatherDimensionNumbers(
            offset_dims=(),
            collapsed_slice_dims=(1,),
            start_index_map=(1,),
            operand_batching_dims=(0,),
            start_indices_batching_dims=(0,),
        ),
        slice_sizes=(1, 1),
        mode=lax.GatherScatterMode.PROMISE_IN_BOUNDS,
    )


def pack_kernel(src_ref, other_src_ref, active_ref, points_ref, index_ref, other_index_ref, *outs):
    half = lax.axis_index("rep")
    row = lax.broadcasted_iota(jnp.int32, (SUBLANES, LANES), 0)
    for m, out in enumerate(outs):
        k = 2 * m + 1 - half
        parts = ((src_ref, index_ref, half), (other_src_ref, other_index_ref, 1 - half))
        for h, (src, index, part) in enumerate(parts):
            for j in range(SUBLANES):
                b = src[k, j]
                for c in range(3):
                    out[c, pl.ds(h * SUBLANES + j, 1), :] = points_ref[c, pl.ds(b, 1), :]
            live = row + part * SUBLANES < active_ref[0, k]
            out[3, pl.ds(h * SUBLANES, SUBLANES), :] = jnp.where(live, index[k], -1).astype(jnp.float32)


def pair_kernel(points_ref, normals_ref, message_ref, *refs):
    (previous_ref,) = refs[:-3] or (None,)
    row_ref, total_ref, sums_s = refs[-3:]
    shape = (SUBLANES, LANES)
    index = [message_ref[3, pl.ds(h * SUBLANES, SUBLANES), :].astype(jnp.int32) for h in range(2)]
    lanes = [i & (LANES - 1) for i in index]
    high = [i >> 7 for i in index]
    found = [[jnp.zeros(shape, jnp.float32) for _ in range(6)] for _ in range(2)]
    for r in range(points_ref.shape[1]):
        here = [h == r for h in high]
        for c in range(6):
            table = points_ref if c < 3 else normals_ref
            line = jnp.broadcast_to(table[c % 3, pl.ds(r, 1), :], shape)
            for h in range(2):
                found[h][c] = jnp.where(here[h], pick_lanes(line, lanes[h]), found[h][c])
    parts = []
    for h in range(2):
        p = [message_ref[c, pl.ds(h * SUBLANES, SUBLANES), :] for c in range(3)]
        q, n = found[h][:3], found[h][3:]
        resid = n[0] * (p[0] - q[0]) + n[1] * (p[1] - q[1]) + n[2] * (p[2] - q[2])
        weight = 1.0 / (1.0 + resid * resid)
        jacob = [
            p[1] * n[2] - p[2] * n[1],
            p[2] * n[0] - p[0] * n[2],
            p[0] * n[1] - p[1] * n[0],
            n[0],
            n[1],
            n[2],
        ]
        scaled = [weight * x for x in jacob]
        terms = [scaled[a] * jacob[b] for a in range(6) for b in range(a, 6)]
        terms += [scaled[a] * resid for a in range(6)]
        parts.append(terms)
    for t in range(27):
        sums_s[pl.ds(t, 1), :] = jnp.sum(parts[0][t] + parts[1][t], axis=0, keepdims=True)

    row = lax.broadcasted_iota(jnp.int32, shape, 0)
    lane = lax.broadcasted_iota(jnp.int32, shape, 1)
    first, second = lane // 6, lane % 6
    low, top = jnp.minimum(first, second), jnp.maximum(first, second)
    gram_term = jnp.where(lane < 36, low * (11 - low) // 2 + top, -1)
    push_term = jnp.where(lane < 6, 21 + lane, -1)
    gram = jnp.zeros(shape, jnp.float32)
    push = jnp.zeros(shape, jnp.float32)
    for g in range(4):
        column = jnp.sum(sums_s[pl.ds(SUBLANES * g, SUBLANES), :], axis=1, keepdims=True)
        term = SUBLANES * g + row
        if g < 3:
            gram = jnp.where(gram_term == term, column, gram)
        if g > 1:
            push = jnp.where(push_term == term, column, push)
    scale = 1.0 / (NB * BLOCK)
    gram = jnp.sum(gram, axis=0, keepdims=True) * scale
    push = jnp.sum(push, axis=0, keepdims=True) * scale
    row_ref[0:1, :] = gram
    row_ref[1:2, :] = push
    if previous_ref is not None:
        gram = previous_ref[0:1, :] + gram
        push = previous_ref[1:2, :] - push
    else:
        push = -push
    total_ref[0:1, :] = gram
    total_ref[1:2, :] = push


def finish_kernel(*refs, scale):
    rows, totals, (diag_ref, grad_ref, pair_ref) = refs[:8], refs[8:10], refs[10:]
    half = lax.axis_index("rep")
    total = totals[0][...] + totals[1][...]
    for i in range(8):
        m, other = i % 4, i // 4
        k = 2 * m + half if other else 2 * m + 1 - half
        got = rows[i][...]
        pair_ref[pl.ds(k, 1), :] = got[0:1, :36]
        total = total + got
    diag_ref[...] = total[0:1, :36] * scale
    grad_ref[...] = total[1:2, :6] * scale


def body(points, normals, src_block, tgt_index, active, *, blk):
    rounds = src_block.shape[0]
    table = (3, points.shape[2] // LANES, LANES)
    points = near(points.reshape(table))
    normals = near(normals.reshape(table))
    src = src_block.reshape(rounds, SUBLANES)
    index = tgt_index.reshape(rounds, SUBLANES, BLOCK)
    f32 = jnp.float32
    messages = pl.pallas_call(
        pack_kernel,
        in_specs=[SMEM, SMEM, SMEM, VMEM, VMEM, VMEM],
        out_specs=[VMEM] * 4,
        out_shape=[pltpu.VMEM((4, NB, LANES), f32)] * 4,
        name="pack",
    )(src, swapped(src), active.reshape(1, rounds), points, near(index), near(swapped(index)))
    offsets = [(2 * m + 2, 2 * m + 1) for m in range(4)]
    there = [routed(x, blk, (-even, -odd)) for x, (even, odd) in zip(messages, offsets)]
    pair = functools.partial(
        pl.pallas_call,
        pair_kernel,
        out_specs=[VMEM] * 2,
        out_shape=[pltpu.VMEM((2, LANES), f32)] * 2,
        scratch_shapes=[pltpu.VMEM((32, LANES), f32)],
        name="pair",
    )
    rows, total = [], []
    for m in range(4):
        row, last = pair(in_specs=[VMEM] * (3 + len(total)))(
            points, normals, near(there[m]), *(near(x) for x in total)
        )
        rows.append(row)
        total = [last]
    back = [routed(x, blk, pair_offsets) for x, pair_offsets in zip(rows, offsets)]
    others = [swapped(x) for x in back]
    diag, grad, pairs = pl.pallas_call(
        functools.partial(finish_kernel, scale=1.0 / (2.0 * rounds)),
        in_specs=[VMEM] * 10,
        out_specs=[VMEM] * 3,
        out_shape=[
            jax.ShapeDtypeStruct((1, 36), f32),
            jax.ShapeDtypeStruct((1, 6), f32),
            jax.ShapeDtypeStruct((rounds, 36), f32),
        ],
        name="finish",
    )(*(near(x) for x in (*back, *others, total[0], swapped(total[0]))))
    return diag, grad, pairs.reshape(rounds, 1, 1, 36)


def solution(mesh):
    return jax.shard_map(
        functools.partial(body, blk=mesh.shape["blk"]),
        mesh=mesh,
        in_specs=(
            P("blk", None, None),
            P("blk", None, None),
            P(None, "blk", None, "rep"),
            P(None, "blk", None, "rep", None),
            P(None, "blk", None),
        ),
        out_specs=(P("blk", None), P("blk", None), P(None, "blk", None, None)),
        check_vma=False,
    )
```

```python
import functools

import jax
import jax.numpy as jnp
from jax import lax
from jax.experimental import pallas as pl
from jax.experimental.pallas import tpu as pltpu
from jax.sharding import PartitionSpec as P

NB = 16
BLOCK = 128
LANES = 128
SUBLANES = 8
FAR = 4


VMEM = pl.BlockSpec(memory_space=pltpu.VMEM)
SMEM = pl.BlockSpec(memory_space=pltpu.SMEM)


def routed(block, blk, shifts):
    route = [(i * 2 + r, (i + shifts[r]) % blk * 2 + r) for i in range(blk) for r in range(2)]
    return lax.ppermute(block, ("blk", "rep"), route)


def swapped(block):
    return lax.ppermute(block, "rep", [(0, 1), (1, 0)])


def near(x):
    return pltpu.with_memory_space_constraint(x, pltpu.VMEM)


def pick_lanes(row, lanes):
    return lax.gather(
        row,
        lanes[:, :, None],
        lax.GatherDimensionNumbers(
            offset_dims=(),
            collapsed_slice_dims=(1,),
            start_index_map=(1,),
            operand_batching_dims=(0,),
            start_indices_batching_dims=(0,),
        ),
        slice_sizes=(1, 1),
        mode=lax.GatherScatterMode.PROMISE_IN_BOUNDS,
    )


def pack_kernel(src_ref, active_ref, points_ref, index_ref, *outs):
    half = lax.axis_index("rep")
    slot = lax.broadcasted_iota(jnp.int32, (SUBLANES, LANES), 0) + half * SUBLANES
    for other, out in enumerate(outs):
        for n in range(4):
            k = 2 * n + half if other else 2 * n + 1 - half
            for j in range(SUBLANES):
                b = src_ref[k, j]
                for c in range(3):
                    out[n, c, pl.ds(j, 1), :] = points_ref[c, pl.ds(b, 1), :]
            live = slot < active_ref[0, k]
            out[n, 3] = jnp.where(live, index_ref[k], -1).astype(jnp.float32)


def merge_kernel(own_ref, other_ref, *outs):
    for m, out in enumerate(outs):
        for j in range(2):
            for c in range(4):
                out[j, c, pl.ds(0, SUBLANES), :] = own_ref[m + 2 * j, c]
                out[j, c, pl.ds(SUBLANES, SUBLANES), :] = other_ref[m + 2 * j, c]


def pair_kernel(points_ref, normals_ref, message_ref, *refs, which, has_rows, has_total):
    refs = list(refs)
    rows_ref = refs.pop(0) if has_rows else None
    previous_ref = refs.pop(0) if has_total else None
    out_ref, total_ref, sums_s = refs
    shape = (SUBLANES, LANES)
    index = [message_ref[which, 3, pl.ds(h * SUBLANES, SUBLANES), :].astype(jnp.int32) for h in range(2)]
    lanes = [i & (LANES - 1) for i in index]
    high = [i >> 7 for i in index]
    found = [[jnp.zeros(shape, jnp.float32) for _ in range(6)] for _ in range(2)]
    for r in range(points_ref.shape[1]):
        here = [h == r for h in high]
        for c in range(6):
            table = points_ref if c < 3 else normals_ref
            line = jnp.broadcast_to(table[c % 3, pl.ds(r, 1), :], shape)
            for h in range(2):
                found[h][c] = jnp.where(here[h], pick_lanes(line, lanes[h]), found[h][c])
    parts = []
    for h in range(2):
        p = [message_ref[which, c, pl.ds(h * SUBLANES, SUBLANES), :] for c in range(3)]
        q, n = found[h][:3], found[h][3:]
        resid = n[0] * (p[0] - q[0]) + n[1] * (p[1] - q[1]) + n[2] * (p[2] - q[2])
        weight = 1.0 / (1.0 + resid * resid)
        jacob = [
            p[1] * n[2] - p[2] * n[1],
            p[2] * n[0] - p[0] * n[2],
            p[0] * n[1] - p[1] * n[0],
            n[0],
            n[1],
            n[2],
        ]
        scaled = [weight * x for x in jacob]
        terms = [scaled[a] * jacob[b] for a in range(6) for b in range(a, 6)]
        terms += [scaled[a] * resid for a in range(6)]
        parts.append(terms)
    for t in range(27):
        sums_s[pl.ds(t, 1), :] = jnp.sum(parts[0][t] + parts[1][t], axis=0, keepdims=True)

    row = lax.broadcasted_iota(jnp.int32, shape, 0)
    lane = lax.broadcasted_iota(jnp.int32, shape, 1)
    first, second = lane // 6, lane % 6
    low, top = jnp.minimum(first, second), jnp.maximum(first, second)
    gram_term = jnp.where(lane < 36, low * (11 - low) // 2 + top, -1)
    push_term = jnp.where(lane < 6, 21 + lane, -1)
    gram = jnp.zeros(shape, jnp.float32)
    push = jnp.zeros(shape, jnp.float32)
    for g in range(4):
        column = jnp.sum(sums_s[pl.ds(SUBLANES * g, SUBLANES), :], axis=1, keepdims=True)
        term = SUBLANES * g + row
        if g < 3:
            gram = jnp.where(gram_term == term, column, gram)
        if g > 1:
            push = jnp.where(push_term == term, column, push)
    scale = 1.0 / (NB * BLOCK)
    gram = jnp.sum(gram, axis=0, keepdims=True) * scale
    push = jnp.sum(push, axis=0, keepdims=True) * scale
    first_row = 0
    if has_rows:
        out_ref[0:2, :] = rows_ref[...]
        first_row = 2
    out_ref[first_row : first_row + 1, :] = gram
    out_ref[first_row + 1 : first_row + 2, :] = push
    if has_total:
        gram = previous_ref[0:1, :] + gram
        push = previous_ref[1:2, :] - push
    else:
        push = -push
    total_ref[0:1, :] = gram
    total_ref[1:2, :] = push


def finish_kernel(*refs, scale):
    rows, totals, (diag_ref, grad_ref, pair_ref) = refs[:4], refs[4:8], refs[8:]
    half = lax.axis_index("rep")
    total = (totals[0][...] + totals[1][...]) + (totals[2][...] + totals[3][...])
    for i in range(4):
        m, other = i % 2, i // 2
        for j in range(2):
            k = 2 * m + FAR * j + (half if other else 1 - half)
            got = rows[i][2 * j : 2 * j + 2, :]
            pair_ref[pl.ds(k, 1), :] = got[0:1, :36]
            total = total + got
    diag_ref[...] = total[0:1, :36] * scale
    grad_ref[...] = total[1:2, :6] * scale


def body(points, normals, src_block, tgt_index, active, *, blk):
    rounds = src_block.shape[0]
    table = (3, points.shape[2] // LANES, LANES)
    points = points.reshape(table)
    normals = normals.reshape(table)
    src = src_block.reshape(rounds, SUBLANES)
    index = tgt_index.reshape(rounds, SUBLANES, BLOCK)
    f32 = jnp.float32
    steps = [(2 * m + 2, 2 * m + 1) for m in range(2)]
    own, other = pl.pallas_call(
        pack_kernel,
        in_specs=[SMEM, SMEM, VMEM, VMEM],
        out_specs=[VMEM] * 2,
        out_shape=[pltpu.VMEM((4, 4, SUBLANES, LANES), f32)] * 2,
        name="pack",
    )(src, active.reshape(1, rounds), points, index)
    far_points = routed(points, blk, (FAR, FAR))
    messages = pl.pallas_call(
        merge_kernel,
        in_specs=[VMEM] * 2,
        out_specs=[VMEM] * 2,
        out_shape=[pltpu.VMEM((2, 4, NB, LANES), f32)] * 2,
        name="merge",
    )(near(own), near(swapped(other)))
    far_normals = routed(normals, blk, (FAR, FAR))
    there = [routed(x, blk, (-even, -odd)) for x, (even, odd) in zip(messages, steps)]

    def pair(tables, message, which, rows=None, total=None):
        extra = [x for x in (rows, total) if x is not None]
        return pl.pallas_call(
            functools.partial(pair_kernel, which=which, has_rows=rows is not None, has_total=total is not None),
            in_specs=[VMEM] * (3 + len(extra)),
            out_specs=[VMEM] * 2,
            out_shape=[pltpu.VMEM((2 if rows is None else 4, LANES), f32), pltpu.VMEM((2, LANES), f32)],
            scratch_shapes=[pltpu.VMEM((32, LANES), f32)],
            name="pair",
        )(*(near(x) for x in (*tables, message, *extra)))

    here, far = (points, normals), (far_points, far_normals)
    rows0, total = pair(here, there[0], 0)
    rows1, total = pair(here, there[1], 0, total=total)
    rows0, far_total = pair(far, there[0], 1, rows=rows0)
    rows1, far_total = pair(far, there[1], 1, rows=rows1, total=far_total)
    back = [routed(x, blk, step) for x, step in zip((rows0, rows1), steps)]
    far_total = routed(far_total, blk, (-FAR, -FAR))
    diag, grad, pairs = pl.pallas_call(
        functools.partial(finish_kernel, scale=1.0 / (2.0 * rounds)),
        in_specs=[VMEM] * 8,
        out_specs=[VMEM] * 3,
        out_shape=[
            jax.ShapeDtypeStruct((1, 36), f32),
            jax.ShapeDtypeStruct((1, 6), f32),
            jax.ShapeDtypeStruct((rounds, 36), f32),
        ],
        name="finish",
    )(*(near(x) for x in (*back, *map(swapped, back), total, swapped(total), far_total, swapped(far_total))))
    return diag, grad, pairs.reshape(rounds, 1, 1, 36)


def solution(mesh):
    return jax.shard_map(
        functools.partial(body, blk=mesh.shape["blk"]),
        mesh=mesh,
        in_specs=(
            P("blk", None, None),
            P("blk", None, None),
            P(None, "blk", None, "rep"),
            P(None, "blk", None, "rep", None),
            P(None, "blk", None),
        ),
        out_specs=(P("blk", None), P("blk", None), P(None, "blk", None, None)),
        check_vma=False,
    )
```

```python
import functools

import jax
import jax.numpy as jnp
from jax import lax
from jax.experimental import pallas as pl
from jax.experimental.pallas import tpu as pltpu
from jax.sharding import PartitionSpec as P


NB = 16
BLOCK = 128
LANES = 128
SUBLANES = 8
FAR = 4


VMEM = pl.BlockSpec(memory_space=pltpu.VMEM)
SMEM = pl.BlockSpec(memory_space=pltpu.SMEM)


def routed(block, blk, shifts):
    route = [(i * 2 + r, (i + shifts[r]) % blk * 2 + r) for i in range(blk) for r in range(2)]
    return lax.ppermute(block, ("blk", "rep"), route)


def swapped(block):
    return lax.ppermute(block, "rep", [(0, 1), (1, 0)])


def near(x):
    return pltpu.with_memory_space_constraint(x, pltpu.VMEM)


def pick_lanes(row, lanes):
    return lax.gather(
        row,
        lanes[:, :, None],
        lax.GatherDimensionNumbers(
            offset_dims=(),
            collapsed_slice_dims=(1,),
            start_index_map=(1,),
            operand_batching_dims=(0,),
            start_indices_batching_dims=(0,),
        ),
        slice_sizes=(1, 1),
        mode=lax.GatherScatterMode.PROMISE_IN_BOUNDS,
    )


def step_of(m, rep):
    return 3 - 3 * rep if m else 1 + rep


def pack_kernel(src_ref, active_ref, points_ref, normals_ref, index_ref, table_ref, *outs):
    half = lax.axis_index("rep")
    slot = lax.broadcasted_iota(jnp.int32, (SUBLANES, LANES), 0) + half * SUBLANES
    for other, out in enumerate(outs):
        for m in range(2):
            for far in range(2):
                k = step_of(m, 1 - half if other else half) + FAR * far
                for j in range(SUBLANES):
                    b = src_ref[k, j]
                    for c in range(3):
                        out[m, far, c, pl.ds(j, 1), :] = points_ref[c, pl.ds(b, 1), :]
                live = slot < active_ref[0, k]
                out[m, far, 3] = jnp.where(live, index_ref[k], -1).astype(jnp.float32)
    table_ref[0:3] = points_ref[...]
    table_ref[3:6] = normals_ref[...]


def merge_kernel(own_ref, other_ref, *outs):
    for m, out in enumerate(outs):
        for far in range(2):
            for c in range(4):
                out[far, c, pl.ds(0, SUBLANES), :] = own_ref[m, far, c]
                out[far, c, pl.ds(SUBLANES, SUBLANES), :] = other_ref[m, far, c]


def pair_kernel(table_ref, far_ref, message_ref, *refs):
    (previous_ref,) = refs[:-3] or (None,)
    rows_ref, totals_ref, sums_s = refs[-3:]
    shape = (SUBLANES, LANES)
    for far, table in enumerate((table_ref, far_ref)):
        index = [message_ref[far, 3, pl.ds(h * SUBLANES, SUBLANES), :].astype(jnp.int32) for h in range(2)]
        lanes = [i & (LANES - 1) for i in index]
        high = [i >> 7 for i in index]
        found = [[jnp.zeros(shape, jnp.float32) for _ in range(6)] for _ in range(2)]
        for r in range(table.shape[1]):
            here = [h == r for h in high]
            for c in range(6):
                line = jnp.broadcast_to(table[c, pl.ds(r, 1), :], shape)
                for h in range(2):
                    found[h][c] = jnp.where(here[h], pick_lanes(line, lanes[h]), found[h][c])
        parts = []
        for h in range(2):
            p = [message_ref[far, c, pl.ds(h * SUBLANES, SUBLANES), :] for c in range(3)]
            q, n = found[h][:3], found[h][3:]
            resid = n[0] * (p[0] - q[0]) + n[1] * (p[1] - q[1]) + n[2] * (p[2] - q[2])
            weight = 1.0 / (1.0 + resid * resid)
            jacob = [
                p[1] * n[2] - p[2] * n[1],
                p[2] * n[0] - p[0] * n[2],
                p[0] * n[1] - p[1] * n[0],
                n[0],
                n[1],
                n[2],
            ]
            scaled = [weight * x for x in jacob]
            terms = [scaled[a] * jacob[b] for a in range(6) for b in range(a, 6)]
            terms += [scaled[a] * resid for a in range(6)]
            parts.append(terms)
        for t in range(27):
            sums_s[far, pl.ds(t, 1), :] = jnp.sum(parts[0][t] + parts[1][t], axis=0, keepdims=True)

    row = lax.broadcasted_iota(jnp.int32, shape, 0)
    lane = lax.broadcasted_iota(jnp.int32, shape, 1)
    first, second = lane // 6, lane % 6
    low, top = jnp.minimum(first, second), jnp.maximum(first, second)
    gram_term = jnp.where(lane < 36, low * (11 - low) // 2 + top, -1)
    push_term = jnp.where(lane < 6, 21 + lane, -1)
    scale = 1.0 / (NB * BLOCK)
    for far in range(2):
        gram = jnp.zeros(shape, jnp.float32)
        push = jnp.zeros(shape, jnp.float32)
        for g in range(4):
            column = jnp.sum(sums_s[far, pl.ds(SUBLANES * g, SUBLANES), :], axis=1, keepdims=True)
            term = SUBLANES * g + row
            if g < 3:
                gram = jnp.where(gram_term == term, column, gram)
            if g > 1:
                push = jnp.where(push_term == term, column, push)
        gram = jnp.sum(gram, axis=0, keepdims=True) * scale
        push = jnp.sum(push, axis=0, keepdims=True) * scale
        at = 2 * far
        rows_ref[at : at + 1, :] = gram
        rows_ref[at + 1 : at + 2, :] = push
        push = -push
        if previous_ref is not None:
            gram = previous_ref[at : at + 1, :] + gram
            push = previous_ref[at + 1 : at + 2, :] + push
        totals_ref[at : at + 1, :] = gram
        totals_ref[at + 1 : at + 2, :] = push


def join_kernel(own_ref, other_ref, here_ref, far_ref):
    here_ref[...] = own_ref[0:2, :] + other_ref[0:2, :]
    far_ref[...] = own_ref[2:4, :] + other_ref[2:4, :]


def finish_kernel(*refs, scale):
    rows, totals, (diag_ref, grad_ref, pair_ref) = refs[:4], refs[4:6], refs[6:]
    half = lax.axis_index("rep")
    total = totals[0][...] + totals[1][...]
    for i in range(4):
        m, other = i % 2, i // 2
        for far in range(2):
            k = step_of(m, 1 - half if other else half) + FAR * far
            got = rows[i][2 * far : 2 * far + 2, :]
            pair_ref[pl.ds(k, 1), :] = got[0:1, :36]
            total = total + got
    diag_ref[...] = total[0:1, :36] * scale
    grad_ref[...] = total[1:2, :6] * scale


def body(points, normals, src_block, tgt_index, active, *, blk):
    rounds = src_block.shape[0]
    scan = (3, points.shape[2] // LANES, LANES)
    f32 = jnp.float32
    steps = [tuple(step_of(m, rep) + 1 for rep in range(2)) for m in range(2)]
    table, own, other = pl.pallas_call(
        pack_kernel,
        in_specs=[SMEM, SMEM, VMEM, VMEM, VMEM],
        out_specs=[VMEM] * 3,
        out_shape=[pltpu.VMEM((6, *scan[1:]), f32)] + [pltpu.VMEM((2, 2, 4, SUBLANES, LANES), f32)] * 2,
        name="pack",
    )(
        src_block.reshape(rounds, SUBLANES),
        active.reshape(1, rounds),
        points.reshape(scan),
        normals.reshape(scan),
        tgt_index.reshape(rounds, SUBLANES, BLOCK),
    )
    other = swapped(other)
    far = routed(table, blk, (FAR, FAR))
    messages = pl.pallas_call(
        merge_kernel,
        in_specs=[VMEM] * 2,
        out_specs=[VMEM] * 2,
        out_shape=[pltpu.VMEM((2, 4, NB, LANES), f32)] * 2,
        name="merge",
    )(near(own), near(other))
    there = [routed(x, blk, tuple(-s for s in step)) for x, step in zip(messages, steps)]
    back, totals = [], []
    for message, step in zip(there, steps):
        rows, last = pl.pallas_call(
            pair_kernel,
            in_specs=[VMEM] * (3 + len(totals)),
            out_specs=[VMEM] * 2,
            out_shape=[pltpu.VMEM((4, LANES), f32)] * 2,
            scratch_shapes=[pltpu.VMEM((2, 32, LANES), f32)],
            name="pair",
        )(*(near(x) for x in (table, far, message, *totals)))
        totals = [last]
        back.append(routed(rows, blk, step))
    other_total = swapped(totals[0])
    here_total, far_total = pl.pallas_call(
        join_kernel,
        in_specs=[VMEM] * 2,
        out_specs=[VMEM] * 2,
        out_shape=[pltpu.VMEM((2, LANES), f32)] * 2,
        name="join",
    )(near(totals[0]), near(other_total))
    far_total = routed(far_total, blk, (-FAR, -FAR))
    others = []
    for x in back:
        others.append(swapped(x))
    diag, grad, pairs = pl.pallas_call(
        functools.partial(finish_kernel, scale=1.0 / (2.0 * rounds)),
        in_specs=[VMEM] * 6,
        out_specs=[VMEM] * 3,
        out_shape=[
            jax.ShapeDtypeStruct((1, 36), f32),
            jax.ShapeDtypeStruct((1, 6), f32),
            jax.ShapeDtypeStruct((rounds, 36), f32),
        ],
        name="finish",
    )(*(near(x) for x in (*back, *others, here_total, far_total)))
    return diag, grad, pairs.reshape(rounds, 1, 1, 36)


def solution(mesh):
    return jax.shard_map(
        functools.partial(body, blk=mesh.shape["blk"]),
        mesh=mesh,
        in_specs=(
            P("blk", None, None),
            P("blk", None, None),
            P(None, "blk", None, "rep"),
            P(None, "blk", None, "rep", None),
            P(None, "blk", None),
        ),
        out_specs=(P("blk", None), P("blk", None), P(None, "blk", None, None)),
        check_vma=False,
    )
```

```python
import functools

import jax
import jax.numpy as jnp
from jax import lax
from jax.experimental import pallas as pl
from jax.experimental.pallas import tpu as pltpu
from jax.sharding import PartitionSpec as P


NB = 16
BLOCK = 128
LANES = 128
SUBLANES = 8
FAR = 4


VMEM = pl.BlockSpec(memory_space=pltpu.VMEM)
SMEM = pl.BlockSpec(memory_space=pltpu.SMEM)


def routed(block, blk, shifts, cross=False):
    route = [(i * 2 + (1 - r if cross else r), (i + shifts[r]) % blk * 2 + r) for i in range(blk) for r in range(2)]
    return lax.ppermute(block, ("blk", "rep"), route)


def swapped(block):
    return lax.ppermute(block, "rep", [(0, 1), (1, 0)])


def near(x):
    return pltpu.with_memory_space_constraint(x, pltpu.VMEM)


def pick_lanes(row, lanes):
    return lax.gather(
        row,
        lanes[:, :, None],
        lax.GatherDimensionNumbers(
            offset_dims=(),
            collapsed_slice_dims=(1,),
            start_index_map=(1,),
            operand_batching_dims=(0,),
            start_indices_batching_dims=(0,),
        ),
        slice_sizes=(1, 1),
        mode=lax.GatherScatterMode.PROMISE_IN_BOUNDS,
    )


def step_of(m, rep):
    return 3 - rep if m else rep


def pack_kernel(src_ref, active_ref, points_ref, normals_ref, index_ref, table_ref, *outs):
    half = lax.axis_index("rep")
    slot = lax.broadcasted_iota(jnp.int32, (SUBLANES, LANES), 0) + half * SUBLANES
    for i, out in enumerate(outs):
        m, cross = i // 2, i % 2
        for far in range(2):
            k = step_of(m, 1 - half if cross else half) + FAR * far
            for j in range(SUBLANES):
                b = src_ref[k, j]
                for c in range(3):
                    out[far, c, pl.ds(j, 1), :] = points_ref[c, pl.ds(b, 1), :]
            live = slot < active_ref[0, k]
            out[far, 3] = jnp.where(live, index_ref[k], -1).astype(jnp.float32)
    table_ref[0:3] = points_ref[...]
    table_ref[3:6] = normals_ref[...]


def pair_kernel(table_ref, first_ref, second_ref, *refs, far):
    rows_ref, totals_ref, sums_s = refs[-3:]
    shape = (SUBLANES, LANES)
    halves = (first_ref, second_ref)
    index = [halves[h][far, 3].astype(jnp.int32) for h in range(2)]
    lanes = [i & (LANES - 1) for i in index]
    high = [i >> 7 for i in index]
    found = [[jnp.zeros(shape, jnp.float32) for _ in range(6)] for _ in range(2)]
    for r in range(table_ref.shape[1]):
        here = [h == r for h in high]
        for c in range(6):
            line = jnp.broadcast_to(table_ref[c, pl.ds(r, 1), :], shape)
            for h in range(2):
                found[h][c] = jnp.where(here[h], pick_lanes(line, lanes[h]), found[h][c])
    parts = []
    for h in range(2):
        p = [halves[h][far, c] for c in range(3)]
        q, n = found[h][:3], found[h][3:]
        resid = n[0] * (p[0] - q[0]) + n[1] * (p[1] - q[1]) + n[2] * (p[2] - q[2])
        weight = 1.0 / (1.0 + resid * resid)
        jacob = [
            p[1] * n[2] - p[2] * n[1],
            p[2] * n[0] - p[0] * n[2],
            p[0] * n[1] - p[1] * n[0],
            n[0],
            n[1],
            n[2],
        ]
        scaled = [weight * x for x in jacob]
        terms = [scaled[a] * jacob[b] for a in range(6) for b in range(a, 6)]
        terms += [scaled[a] * resid for a in range(6)]
        parts.append(terms)
    for t in range(27):
        sums_s[pl.ds(t, 1), :] = jnp.sum(parts[0][t] + parts[1][t], axis=0, keepdims=True)

    row = lax.broadcasted_iota(jnp.int32, shape, 0)
    lane = lax.broadcasted_iota(jnp.int32, shape, 1)
    first, second = lane // 6, lane % 6
    low, top = jnp.minimum(first, second), jnp.maximum(first, second)
    gram_term = jnp.where(lane < 36, low * (11 - low) // 2 + top, -1)
    push_term = jnp.where(lane < 6, 21 + lane, -1)
    gram = jnp.zeros(shape, jnp.float32)
    push = jnp.zeros(shape, jnp.float32)
    for g in range(4):
        column = jnp.sum(sums_s[pl.ds(SUBLANES * g, SUBLANES), :], axis=1, keepdims=True)
        term = SUBLANES * g + row
        if g < 3:
            gram = jnp.where(gram_term == term, column, gram)
        if g > 1:
            push = jnp.where(push_term == term, column, push)
    scale = 1.0 / (NB * BLOCK)
    gram = jnp.sum(gram, axis=0, keepdims=True) * scale
    push = jnp.sum(push, axis=0, keepdims=True) * scale
    at = 2 * far
    if far:
        rows_ref[0:2, :] = refs[1][...]
    rows_ref[at : at + 1, :] = gram
    rows_ref[at + 1 : at + 2, :] = push
    totals_ref[...] = refs[0][...] if len(refs) > 3 else jnp.zeros((4, LANES), jnp.float32)
    totals_ref[at : at + 1, :] += gram
    totals_ref[at + 1 : at + 2, :] -= push


def join_kernel(own_ref, other_ref, here_ref, far_ref):
    here_ref[...] = own_ref[0:2, :] + other_ref[0:2, :]
    far_ref[...] = own_ref[2:4, :] + other_ref[2:4, :]


def finish_kernel(*refs, scale):
    rows, totals, (diag_ref, grad_ref, pair_ref) = refs[:4], refs[4:6], refs[6:]
    half = lax.axis_index("rep")
    total = totals[0][...] + totals[1][...]
    for i in range(4):
        m, other = i % 2, i // 2
        for far in range(2):
            k = step_of(m, 1 - half if other else half) + FAR * far
            got = rows[i][2 * far : 2 * far + 2, :]
            pair_ref[pl.ds(k, 1), :] = got[0:1, :36]
            total = total + got
    diag_ref[...] = total[0:1, :36] * scale
    grad_ref[...] = total[1:2, :6] * scale


def body(points, normals, src_block, tgt_index, active, *, blk):
    rounds = src_block.shape[0]
    scan = (3, points.shape[2] // LANES, LANES)
    f32 = jnp.float32
    steps = [tuple(step_of(m, rep) + 1 for rep in range(2)) for m in range(2)]
    table, *messages = pl.pallas_call(
        pack_kernel,
        in_specs=[SMEM, SMEM, VMEM, VMEM, VMEM],
        out_specs=[VMEM] * 5,
        out_shape=[pltpu.VMEM((6, *scan[1:]), f32)] + [pltpu.VMEM((2, 4, SUBLANES, LANES), f32)] * 4,
        name="pack",
    )(
        src_block.reshape(rounds, SUBLANES),
        active.reshape(1, rounds),
        points.reshape(scan),
        normals.reshape(scan),
        tgt_index.reshape(rounds, SUBLANES, BLOCK),
    )
    there = []
    for m, step in enumerate(steps):
        down = tuple(-s for s in step)
        first = routed(messages[2 * m], blk, down)
        there.append((first, routed(messages[2 * m + 1], blk, down, cross=True)))
    far_table = routed(table, blk, (FAR, FAR))
    back, totals = [], []
    for message, step in zip(there, steps):
        rows = []
        for far in range(2):
            args = [far_table if far else table, *message, *totals, *rows]
            *rows, last = pl.pallas_call(
                functools.partial(pair_kernel, far=far),
                in_specs=[VMEM] * len(args),
                out_specs=[VMEM] * 2,
                out_shape=[pltpu.VMEM((2 + 2 * far, LANES), f32), pltpu.VMEM((4, LANES), f32)],
                scratch_shapes=[pltpu.VMEM((32, LANES), f32)],
                name="pair",
            )(*map(near, args))
            totals = [last]
        back.append(routed(rows[0], blk, step))
    other_total = swapped(totals[0])
    here_total, far_total = pl.pallas_call(
        join_kernel,
        in_specs=[VMEM] * 2,
        out_specs=[VMEM] * 2,
        out_shape=[pltpu.VMEM((2, LANES), f32)] * 2,
        name="join",
    )(near(totals[0]), near(other_total))
    far_total = routed(far_total, blk, (-FAR, -FAR))
    others = []
    for x in back:
        others.append(swapped(x))
    diag, grad, pairs = pl.pallas_call(
        functools.partial(finish_kernel, scale=1.0 / (2.0 * rounds)),
        in_specs=[VMEM] * 6,
        out_specs=[VMEM] * 3,
        out_shape=[
            jax.ShapeDtypeStruct((1, 36), f32),
            jax.ShapeDtypeStruct((1, 6), f32),
            jax.ShapeDtypeStruct((rounds, 36), f32),
        ],
        name="finish",
    )(*(near(x) for x in (*back, *others, here_total, far_total)))
    return diag, grad, pairs.reshape(rounds, 1, 1, 36)


def solution(mesh):
    return jax.shard_map(
        functools.partial(body, blk=mesh.shape["blk"]),
        mesh=mesh,
        in_specs=(
            P("blk", None, None),
            P("blk", None, None),
            P(None, "blk", None, "rep"),
            P(None, "blk", None, "rep", None),
            P(None, "blk", None),
        ),
        out_specs=(P("blk", None), P("blk", None), P(None, "blk", None, None)),
        check_vma=False,
    )
```

```python
import functools

import jax
import jax.numpy as jnp
from jax import lax
from jax.experimental import pallas as pl
from jax.experimental.pallas import tpu as pltpu
from jax.sharding import PartitionSpec as P


NB = 16
BLOCK = 128
LANES = 128
SUBLANES = 8
FAR = 4


VMEM = pl.BlockSpec(memory_space=pltpu.VMEM)
SMEM = pl.BlockSpec(memory_space=pltpu.SMEM)


def routed(block, blk, shifts):
    route = [(i * 2 + r, (i + shifts[r]) % blk * 2 + r) for i in range(blk) for r in range(2)]
    return lax.ppermute(block, ("blk", "rep"), route)


def swapped(block):
    return lax.ppermute(block, "rep", [(0, 1), (1, 0)])


def near(x):
    return pltpu.with_memory_space_constraint(x, pltpu.VMEM)


def pick_lanes(row, lanes):
    return lax.gather(
        row,
        lanes[:, :, None],
        lax.GatherDimensionNumbers(
            offset_dims=(),
            collapsed_slice_dims=(1,),
            start_index_map=(1,),
            operand_batching_dims=(0,),
            start_indices_batching_dims=(0,),
        ),
        slice_sizes=(1, 1),
        mode=lax.GatherScatterMode.PROMISE_IN_BOUNDS,
    )


def step_of(m, rep):
    return rep if m else 3 - rep


def pack_kernel(src_ref, active_ref, points_ref, normals_ref, index_ref, table_ref, *outs):
    half = lax.axis_index("rep")
    slot = lax.broadcasted_iota(jnp.int32, (SUBLANES, LANES), 0) + half * SUBLANES
    for other, out in enumerate(outs):
        for m in range(2):
            for far in range(2):
                k = step_of(m, 1 - half if other else half) + FAR * far
                for j in range(SUBLANES):
                    b = src_ref[k, j]
                    for c in range(3):
                        out[m, far, c, pl.ds(j, 1), :] = points_ref[c, pl.ds(b, 1), :]
                live = slot < active_ref[0, k]
                out[m, far, 3] = jnp.where(live, index_ref[k], -1).astype(jnp.float32)
    table_ref[0:3] = points_ref[...]
    table_ref[3:6] = normals_ref[...]


def merge_kernel(own_ref, other_ref, *outs):
    for m, out in enumerate(outs):
        for far in range(2):
            for c in range(4):
                out[far, c, pl.ds(0, SUBLANES), :] = own_ref[m, far, c]
                out[far, c, pl.ds(SUBLANES, SUBLANES), :] = other_ref[m, far, c]


def pair_kernel(table_ref, message_ref, *refs, far):
    rows_ref, totals_ref, sums_s = refs[-3:]
    shape = (SUBLANES, LANES)
    index = [message_ref[far, 3, pl.ds(h * SUBLANES, SUBLANES), :].astype(jnp.int32) for h in range(2)]
    lanes = [i & (LANES - 1) for i in index]
    high = [i >> 7 for i in index]
    found = [[jnp.zeros(shape, jnp.float32) for _ in range(6)] for _ in range(2)]
    for r in range(table_ref.shape[1]):
        here = [h == r for h in high]
        for c in range(6):
            line = jnp.broadcast_to(table_ref[c, pl.ds(r, 1), :], shape)
            for h in range(2):
                found[h][c] = jnp.where(here[h], pick_lanes(line, lanes[h]), found[h][c])
    parts = []
    for h in range(2):
        p = [message_ref[far, c, pl.ds(h * SUBLANES, SUBLANES), :] for c in range(3)]
        q, n = found[h][:3], found[h][3:]
        resid = n[0] * (p[0] - q[0]) + n[1] * (p[1] - q[1]) + n[2] * (p[2] - q[2])
        weight = 1.0 / (1.0 + resid * resid)
        jacob = [
            p[1] * n[2] - p[2] * n[1],
            p[2] * n[0] - p[0] * n[2],
            p[0] * n[1] - p[1] * n[0],
            n[0],
            n[1],
            n[2],
        ]
        scaled = [weight * x for x in jacob]
        terms = [scaled[a] * jacob[b] for a in range(6) for b in range(a, 6)]
        terms += [scaled[a] * resid for a in range(6)]
        parts.append(terms)
    for t in range(27):
        sums_s[pl.ds(t, 1), :] = jnp.sum(parts[0][t] + parts[1][t], axis=0, keepdims=True)

    row = lax.broadcasted_iota(jnp.int32, shape, 0)
    lane = lax.broadcasted_iota(jnp.int32, shape, 1)
    first, second = lane // 6, lane % 6
    low, top = jnp.minimum(first, second), jnp.maximum(first, second)
    gram_term = jnp.where(lane < 36, low * (11 - low) // 2 + top, -1)
    push_term = jnp.where(lane < 6, 21 + lane, -1)
    gram = jnp.zeros(shape, jnp.float32)
    push = jnp.zeros(shape, jnp.float32)
    for g in range(4):
        column = jnp.sum(sums_s[pl.ds(SUBLANES * g, SUBLANES), :], axis=1, keepdims=True)
        term = SUBLANES * g + row
        if g < 3:
            gram = jnp.where(gram_term == term, column, gram)
        if g > 1:
            push = jnp.where(push_term == term, column, push)
    scale = 1.0 / (NB * BLOCK)
    gram = jnp.sum(gram, axis=0, keepdims=True) * scale
    push = jnp.sum(push, axis=0, keepdims=True) * scale
    at = 2 * far
    if far:
        rows_ref[0:2, :] = refs[1][...]
    rows_ref[at : at + 1, :] = gram
    rows_ref[at + 1 : at + 2, :] = push
    totals_ref[...] = refs[0][...] if len(refs) > 3 else jnp.zeros((4, LANES), jnp.float32)
    totals_ref[at : at + 1, :] += gram
    totals_ref[at + 1 : at + 2, :] -= push


def join_kernel(own_ref, other_ref, here_ref, far_ref):
    here_ref[...] = own_ref[0:2, :] + other_ref[0:2, :]
    far_ref[...] = own_ref[2:4, :] + other_ref[2:4, :]


def finish_kernel(*refs, scale):
    rows, totals, (diag_ref, grad_ref, pair_ref) = refs[:4], refs[4:6], refs[6:]
    half = lax.axis_index("rep")
    total = totals[0][...] + totals[1][...]
    for i in range(4):
        m, other = i % 2, i // 2
        for far in range(2):
            k = step_of(m, 1 - half if other else half) + FAR * far
            got = rows[i][2 * far : 2 * far + 2, :]
            pair_ref[pl.ds(k, 1), :] = got[0:1, :36]
            total = total + got
    diag_ref[...] = total[0:1, :36] * scale
    grad_ref[...] = total[1:2, :6] * scale


def body(points, normals, src_block, tgt_index, active, *, blk):
    rounds = src_block.shape[0]
    scan = (3, points.shape[2] // LANES, LANES)
    f32 = jnp.float32
    steps = [tuple(step_of(m, rep) + 1 for rep in range(2)) for m in range(2)]
    table, own, other = pl.pallas_call(
        pack_kernel,
        in_specs=[SMEM, SMEM, VMEM, VMEM, VMEM],
        out_specs=[VMEM] * 3,
        out_shape=[pltpu.VMEM((6, *scan[1:]), f32)] + [pltpu.VMEM((2, 2, 4, SUBLANES, LANES), f32)] * 2,
        name="pack",
    )(
        src_block.reshape(rounds, SUBLANES),
        active.reshape(1, rounds),
        points.reshape(scan),
        normals.reshape(scan),
        tgt_index.reshape(rounds, SUBLANES, BLOCK),
    )
    other = swapped(other)
    far_table = routed(table, blk, (FAR, FAR))
    messages = pl.pallas_call(
        merge_kernel,
        in_specs=[VMEM] * 2,
        out_specs=[VMEM] * 2,
        out_shape=[pltpu.VMEM((2, 4, NB, LANES), f32)] * 2,
        name="merge",
    )(near(own), near(other))
    there = [routed(x, blk, tuple(-s for s in step)) for x, step in zip(messages, steps)]
    back, totals = [], []
    for message, step in zip(there, steps):
        rows = []
        for far in range(2):
            args = [far_table if far else table, message, *totals, *rows]
            *rows, last = pl.pallas_call(
                functools.partial(pair_kernel, far=far),
                in_specs=[VMEM] * len(args),
                out_specs=[VMEM] * 2,
                out_shape=[pltpu.VMEM((2 + 2 * far, LANES), f32), pltpu.VMEM((4, LANES), f32)],
                scratch_shapes=[pltpu.VMEM((32, LANES), f32)],
                name="pair",
            )(*map(near, args))
            totals = [last]
        back.append(routed(rows[0], blk, step))
    other_total = swapped(totals[0])
    here_total, far_total = pl.pallas_call(
        join_kernel,
        in_specs=[VMEM] * 2,
        out_specs=[VMEM] * 2,
        out_shape=[pltpu.VMEM((2, LANES), f32)] * 2,
        name="join",
    )(near(totals[0]), near(other_total))
    far_total = routed(far_total, blk, (-FAR, -FAR))
    others = []
    for x in back:
        others.append(swapped(x))
    diag, grad, pairs = pl.pallas_call(
        functools.partial(finish_kernel, scale=1.0 / (2.0 * rounds)),
        in_specs=[VMEM] * 6,
        out_specs=[VMEM] * 3,
        out_shape=[
            jax.ShapeDtypeStruct((1, 36), f32),
            jax.ShapeDtypeStruct((1, 6), f32),
            jax.ShapeDtypeStruct((rounds, 36), f32),
        ],
        name="finish",
    )(*(near(x) for x in (*back, *others, here_total, far_total)))
    return diag, grad, pairs.reshape(rounds, 1, 1, 36)


def solution(mesh):
    return jax.shard_map(
        functools.partial(body, blk=mesh.shape["blk"]),
        mesh=mesh,
        in_specs=(
            P("blk", None, None),
            P("blk", None, None),
            P(None, "blk", None, "rep"),
            P(None, "blk", None, "rep", None),
            P(None, "blk", None),
        ),
        out_specs=(P("blk", None), P("blk", None), P(None, "blk", None, None)),
        check_vma=False,
    )
```

```python
import functools

import jax
import jax.numpy as jnp
from jax import lax
from jax.experimental import pallas as pl
from jax.experimental.pallas import tpu as pltpu
from jax.sharding import PartitionSpec as P


NB = 16
BLOCK = 128
LANES = 128
SUBLANES = 8
FAR = 4


VMEM = pl.BlockSpec(memory_space=pltpu.VMEM)
SMEM = pl.BlockSpec(memory_space=pltpu.SMEM)


def routed(block, blk, shifts):
    route = [(i * 2 + r, (i + shifts[r]) % blk * 2 + r) for i in range(blk) for r in range(2)]
    return lax.ppermute(block, ("blk", "rep"), route)


def swapped(block):
    return lax.ppermute(block, "rep", [(0, 1), (1, 0)])


def near(x):
    return pltpu.with_memory_space_constraint(x, pltpu.VMEM)


def pick_lanes(row, lanes):
    return lax.gather(
        row,
        lanes[:, :, None],
        lax.GatherDimensionNumbers(
            offset_dims=(),
            collapsed_slice_dims=(1,),
            start_index_map=(1,),
            operand_batching_dims=(0,),
            start_indices_batching_dims=(0,),
        ),
        slice_sizes=(1, 1),
        mode=lax.GatherScatterMode.PROMISE_IN_BOUNDS,
    )


def step_of(m, rep):
    return rep if m else 3 - rep


def pack_kernel(src_ref, active_ref, points_ref, normals_ref, index_ref, table_ref, *outs):
    half = lax.axis_index("rep")
    slot = lax.broadcasted_iota(jnp.int32, (SUBLANES, LANES), 0) + half * SUBLANES
    for other, out in enumerate(outs):
        for m in range(2):
            for far in range(2):
                k = step_of(m, 1 - half if other else half) + FAR * far
                for j in range(SUBLANES):
                    b = src_ref[k, j]
                    for c in range(3):
                        out[m, far, c, pl.ds(j, 1), :] = points_ref[c, pl.ds(b, 1), :]
                live = slot < active_ref[0, k]
                out[m, far, 3] = jnp.where(live, index_ref[k], -1).astype(jnp.float32)
    table_ref[0:3] = points_ref[...]
    table_ref[3:6] = normals_ref[...]


def merge_kernel(own_ref, other_ref, *outs):
    for m, out in enumerate(outs):
        for far in range(2):
            for c in range(4):
                out[far, c, pl.ds(0, SUBLANES), :] = own_ref[m, far, c]
                out[far, c, pl.ds(SUBLANES, SUBLANES), :] = other_ref[m, far, c]


def pair_kernel(table_ref, message_ref, *refs, far):
    rows_ref, totals_ref, sums_s = refs[-3:]
    shape = (SUBLANES, LANES)
    index = [message_ref[far, 3, pl.ds(h * SUBLANES, SUBLANES), :].astype(jnp.int32) for h in range(2)]
    lanes = [i & (LANES - 1) for i in index]
    high = [i >> 7 for i in index]
    found = [[jnp.zeros(shape, jnp.float32) for _ in range(6)] for _ in range(2)]
    for r in range(table_ref.shape[1]):
        here = [h == r for h in high]
        for c in range(6):
            line = jnp.broadcast_to(table_ref[c, pl.ds(r, 1), :], shape)
            for h in range(2):
                found[h][c] = jnp.where(here[h], pick_lanes(line, lanes[h]), found[h][c])
    parts = []
    for h in range(2):
        p = [message_ref[far, c, pl.ds(h * SUBLANES, SUBLANES), :] for c in range(3)]
        q, n = found[h][:3], found[h][3:]
        resid = n[0] * (p[0] - q[0]) + n[1] * (p[1] - q[1]) + n[2] * (p[2] - q[2])
        weight = 1.0 / (1.0 + resid * resid)
        jacob = [
            p[1] * n[2] - p[2] * n[1],
            p[2] * n[0] - p[0] * n[2],
            p[0] * n[1] - p[1] * n[0],
            n[0],
            n[1],
            n[2],
        ]
        scaled = [weight * x for x in jacob]
        terms = [scaled[a] * jacob[b] for a in range(6) for b in range(a, 6)]
        terms += [scaled[a] * resid for a in range(6)]
        parts.append(terms)
    for t in range(27):
        sums_s[pl.ds(t, 1), :] = jnp.sum(parts[0][t] + parts[1][t], axis=0, keepdims=True)

    row = lax.broadcasted_iota(jnp.int32, shape, 0)
    lane = lax.broadcasted_iota(jnp.int32, shape, 1)
    first, second = lane // 6, lane % 6
    low, top = jnp.minimum(first, second), jnp.maximum(first, second)
    gram_term = jnp.where(lane < 36, low * (11 - low) // 2 + top, -1)
    push_term = jnp.where(lane < 6, 21 + lane, -1)
    gram = jnp.zeros(shape, jnp.float32)
    push = jnp.zeros(shape, jnp.float32)
    for g in range(4):
        column = jnp.sum(sums_s[pl.ds(SUBLANES * g, SUBLANES), :], axis=1, keepdims=True)
        term = SUBLANES * g + row
        if g < 3:
            gram = jnp.where(gram_term == term, column, gram)
        if g > 1:
            push = jnp.where(push_term == term, column, push)
    scale = 1.0 / (NB * BLOCK)
    gram = jnp.sum(gram, axis=0, keepdims=True) * scale
    push = jnp.sum(push, axis=0, keepdims=True) * scale
    at = 2 * far
    if far:
        rows_ref[0:2, :] = refs[1][...]
    rows_ref[at : at + 1, :] = gram
    rows_ref[at + 1 : at + 2, :] = push
    totals_ref[...] = refs[0][...] if len(refs) > 3 else jnp.zeros((4, LANES), jnp.float32)
    totals_ref[at : at + 1, :] += gram
    totals_ref[at + 1 : at + 2, :] -= push


def split_kernel(totals_ref, here_ref, far_ref):
    here_ref[...] = totals_ref[0:2, :]
    far_ref[...] = totals_ref[2:4, :]


def join_kernel(here_ref, far_ref, total_ref):
    total_ref[...] = here_ref[...] + far_ref[...]


def finish_kernel(*refs, scale):
    rows, totals, (diag_ref, grad_ref, pair_ref) = refs[:4], refs[4:6], refs[6:]
    half = lax.axis_index("rep")
    total = totals[0][...] + totals[1][...]
    for i in range(4):
        m, other = i % 2, i // 2
        for far in range(2):
            k = step_of(m, 1 - half if other else half) + FAR * far
            got = rows[i][2 * far : 2 * far + 2, :]
            pair_ref[pl.ds(k, 1), :] = got[0:1, :36]
            total = total + got
    diag_ref[...] = total[0:1, :36] * scale
    grad_ref[...] = total[1:2, :6] * scale


def body(points, normals, src_block, tgt_index, active, *, blk):
    rounds = src_block.shape[0]
    scan = (3, points.shape[2] // LANES, LANES)
    f32 = jnp.float32
    steps = [tuple(step_of(m, rep) + 1 for rep in range(2)) for m in range(2)]
    table, own, other = pl.pallas_call(
        pack_kernel,
        in_specs=[SMEM, SMEM, VMEM, VMEM, VMEM],
        out_specs=[VMEM] * 3,
        out_shape=[pltpu.VMEM((6, *scan[1:]), f32)] + [pltpu.VMEM((2, 2, 4, SUBLANES, LANES), f32)] * 2,
        name="pack",
    )(
        src_block.reshape(rounds, SUBLANES),
        active.reshape(1, rounds),
        points.reshape(scan),
        normals.reshape(scan),
        tgt_index.reshape(rounds, SUBLANES, BLOCK),
    )
    other = swapped(other)
    far_table = routed(table, blk, (FAR, FAR))
    messages = pl.pallas_call(
        merge_kernel,
        in_specs=[VMEM] * 2,
        out_specs=[VMEM] * 2,
        out_shape=[pltpu.VMEM((2, 4, NB, LANES), f32)] * 2,
        name="merge",
    )(near(own), near(other))
    there = [routed(x, blk, tuple(-s for s in step)) for x, step in zip(messages, steps)]
    back, totals = [], []
    for message, step in zip(there, steps):
        rows = []
        for far in range(2):
            args = [far_table if far else table, message, *totals, *rows]
            *rows, last = pl.pallas_call(
                functools.partial(pair_kernel, far=far),
                in_specs=[VMEM] * len(args),
                out_specs=[VMEM] * 2,
                out_shape=[pltpu.VMEM((2 + 2 * far, LANES), f32), pltpu.VMEM((4, LANES), f32)],
                scratch_shapes=[pltpu.VMEM((32, LANES), f32)],
                name="pair",
            )(*map(near, args))
            totals = [last]
        back.append(routed(rows[0], blk, step))
    total = pltpu.VMEM((2, LANES), f32)
    here_total, far_total = pl.pallas_call(
        split_kernel, in_specs=[VMEM], out_specs=[VMEM] * 2, out_shape=[total] * 2, name="split"
    )(near(totals[0]))
    far_total = routed(far_total, blk, (-FAR, -FAR))
    total = pl.pallas_call(
        join_kernel, in_specs=[VMEM] * 2, out_specs=VMEM, out_shape=total, name="join"
    )(near(here_total), near(far_total))
    other_total = swapped(total)
    others = []
    for x in back:
        others.append(swapped(x))
    diag, grad, pairs = pl.pallas_call(
        functools.partial(finish_kernel, scale=1.0 / (2.0 * rounds)),
        in_specs=[VMEM] * 6,
        out_specs=[VMEM] * 3,
        out_shape=[
            jax.ShapeDtypeStruct((1, 36), f32),
            jax.ShapeDtypeStruct((1, 6), f32),
            jax.ShapeDtypeStruct((rounds, 36), f32),
        ],
        name="finish",
    )(*(near(x) for x in (*back, *others, total, other_total)))
    return diag, grad, pairs.reshape(rounds, 1, 1, 36)


def solution(mesh):
    return jax.shard_map(
        functools.partial(body, blk=mesh.shape["blk"]),
        mesh=mesh,
        in_specs=(
            P("blk", None, None),
            P("blk", None, None),
            P(None, "blk", None, "rep"),
            P(None, "blk", None, "rep", None),
            P(None, "blk", None),
        ),
        out_specs=(P("blk", None), P("blk", None), P(None, "blk", None, None)),
        check_vma=False,
    )
```

```python
import functools

import jax
import jax.numpy as jnp
from jax import lax
from jax.experimental import pallas as pl
from jax.experimental.pallas import tpu as pltpu
from jax.sharding import PartitionSpec as P


NB = 16
BLOCK = 128
LANES = 128
SUBLANES = 8
FAR = 4


VMEM = pl.BlockSpec(memory_space=pltpu.VMEM)
SMEM = pl.BlockSpec(memory_space=pltpu.SMEM)


def routed(block, blk, shifts, cross=False):
    route = [(i * 2 + r, (i + shifts[r]) % blk * 2 + (1 - r if cross else r)) for i in range(blk) for r in range(2)]
    return lax.ppermute(block, ("blk", "rep"), route)


def swapped(block):
    return lax.ppermute(block, "rep", [(0, 1), (1, 0)])


def near(x):
    return pltpu.with_memory_space_constraint(x, pltpu.VMEM)


def pick_lanes(row, lanes):
    return lax.gather(
        row,
        lanes[:, :, None],
        lax.GatherDimensionNumbers(
            offset_dims=(),
            collapsed_slice_dims=(1,),
            start_index_map=(1,),
            operand_batching_dims=(0,),
            start_indices_batching_dims=(0,),
        ),
        slice_sizes=(1, 1),
        mode=lax.GatherScatterMode.PROMISE_IN_BOUNDS,
    )


def step_of(m, rep):
    return 2 * m + rep


def pack_kernel(src_ref, active_ref, points_ref, normals_ref, index_ref, table_ref, *outs):
    half = lax.axis_index("rep")
    slot = lax.broadcasted_iota(jnp.int32, (SUBLANES, LANES), 0) + half * SUBLANES
    for other, out in enumerate(outs):
        for m in range(2):
            for far in range(2):
                k = step_of(m, 1 - half if other else half) + FAR * far
                for j in range(SUBLANES):
                    b = src_ref[k, j]
                    for c in range(3):
                        out[m, far, c, pl.ds(j, 1), :] = points_ref[c, pl.ds(b, 1), :]
                live = slot < active_ref[0, k]
                out[m, far, 3] = jnp.where(live, index_ref[k], -1).astype(jnp.float32)
    table_ref[0:3] = points_ref[...]
    table_ref[3:6] = normals_ref[...]


def merge_kernel(own_ref, other_ref, *outs):
    for m, out in enumerate(outs):
        for far in range(2):
            for c in range(4):
                out[far, c, pl.ds(0, SUBLANES), :] = own_ref[m, far, c]
                out[far, c, pl.ds(SUBLANES, SUBLANES), :] = other_ref[m, far, c]


def pair_kernel(table_ref, message_ref, *refs, far):
    rows_ref, totals_ref, sums_s = refs[-3:]
    shape = (SUBLANES, LANES)
    index = [message_ref[far, 3, pl.ds(h * SUBLANES, SUBLANES), :].astype(jnp.int32) for h in range(2)]
    lanes = [i & (LANES - 1) for i in index]
    high = [i >> 7 for i in index]
    found = [[jnp.zeros(shape, jnp.float32) for _ in range(6)] for _ in range(2)]
    for r in range(table_ref.shape[1]):
        here = [h == r for h in high]
        for c in range(6):
            line = jnp.broadcast_to(table_ref[c, pl.ds(r, 1), :], shape)
            for h in range(2):
                found[h][c] = jnp.where(here[h], pick_lanes(line, lanes[h]), found[h][c])
    parts = []
    for h in range(2):
        p = [message_ref[far, c, pl.ds(h * SUBLANES, SUBLANES), :] for c in range(3)]
        q, n = found[h][:3], found[h][3:]
        resid = n[0] * (p[0] - q[0]) + n[1] * (p[1] - q[1]) + n[2] * (p[2] - q[2])
        weight = 1.0 / (1.0 + resid * resid)
        jacob = [
            p[1] * n[2] - p[2] * n[1],
            p[2] * n[0] - p[0] * n[2],
            p[0] * n[1] - p[1] * n[0],
            n[0],
            n[1],
            n[2],
        ]
        scaled = [weight * x for x in jacob]
        terms = [scaled[a] * jacob[b] for a in range(6) for b in range(a, 6)]
        terms += [scaled[a] * resid for a in range(6)]
        parts.append(terms)
    for t in range(27):
        sums_s[pl.ds(t, 1), :] = jnp.sum(parts[0][t] + parts[1][t], axis=0, keepdims=True)

    row = lax.broadcasted_iota(jnp.int32, shape, 0)
    lane = lax.broadcasted_iota(jnp.int32, shape, 1)
    first, second = lane // 6, lane % 6
    low, top = jnp.minimum(first, second), jnp.maximum(first, second)
    gram_term = jnp.where(lane < 36, low * (11 - low) // 2 + top, -1)
    push_term = jnp.where(lane < 6, 21 + lane, -1)
    gram = jnp.zeros(shape, jnp.float32)
    push = jnp.zeros(shape, jnp.float32)
    for g in range(4):
        column = jnp.sum(sums_s[pl.ds(SUBLANES * g, SUBLANES), :], axis=1, keepdims=True)
        term = SUBLANES * g + row
        if g < 3:
            gram = jnp.where(gram_term == term, column, gram)
        if g > 1:
            push = jnp.where(push_term == term, column, push)
    scale = 1.0 / (NB * BLOCK)
    gram = jnp.sum(gram, axis=0, keepdims=True) * scale
    push = jnp.sum(push, axis=0, keepdims=True) * scale
    at = 2 * far
    if far:
        rows_ref[0:2, :] = refs[1][...]
    rows_ref[at : at + 1, :] = gram
    rows_ref[at + 1 : at + 2, :] = push
    totals_ref[...] = refs[0][...] if len(refs) > 3 else jnp.zeros((4, LANES), jnp.float32)
    totals_ref[at : at + 1, :] += gram
    totals_ref[at + 1 : at + 2, :] -= push


def join_kernel(own_ref, other_ref, here_ref, far_ref):
    here_ref[...] = own_ref[0:2, :] + other_ref[0:2, :]
    far_ref[...] = own_ref[2:4, :] + other_ref[2:4, :]


def finish_kernel(*refs, scale):
    rows, totals, (diag_ref, grad_ref, pair_ref) = refs[:4], refs[4:6], refs[6:]
    half = lax.axis_index("rep")
    total = totals[0][...] + totals[1][...]
    for i in range(4):
        m, other = i % 2, i // 2
        for far in range(2):
            k = step_of(m, 1 - half if other else half) + FAR * far
            got = rows[i][2 * far : 2 * far + 2, :]
            pair_ref[pl.ds(k, 1), :] = got[0:1, :36]
            total = total + got
    diag_ref[...] = total[0:1, :36] * scale
    grad_ref[...] = total[1:2, :6] * scale


def body(points, normals, src_block, tgt_index, active, *, blk):
    rounds = src_block.shape[0]
    scan = (3, points.shape[2] // LANES, LANES)
    f32 = jnp.float32
    steps = [tuple(step_of(m, rep) + 1 for rep in range(2)) for m in range(2)]
    table, own, other = pl.pallas_call(
        pack_kernel,
        in_specs=[SMEM, SMEM, VMEM, VMEM, VMEM],
        out_specs=[VMEM] * 3,
        out_shape=[pltpu.VMEM((6, *scan[1:]), f32)] + [pltpu.VMEM((2, 2, 4, SUBLANES, LANES), f32)] * 2,
        name="pack",
    )(
        src_block.reshape(rounds, SUBLANES),
        active.reshape(1, rounds),
        points.reshape(scan),
        normals.reshape(scan),
        tgt_index.reshape(rounds, SUBLANES, BLOCK),
    )
    other = swapped(other)
    far_table = routed(table, blk, (FAR, FAR))
    messages = pl.pallas_call(
        merge_kernel,
        in_specs=[VMEM] * 2,
        out_specs=[VMEM] * 2,
        out_shape=[pltpu.VMEM((2, 4, NB, LANES), f32)] * 2,
        name="merge",
    )(near(own), near(other))
    there = []
    for x, step in zip(messages, steps):
        there.append(routed(x, blk, tuple(-s for s in step)))
    back, others, totals = [], [], []
    for message, step in zip(there, steps):
        rows = []
        for far in range(2):
            args = [far_table if far else table, message, *totals, *rows]
            *rows, last = pl.pallas_call(
                functools.partial(pair_kernel, far=far),
                in_specs=[VMEM] * len(args),
                out_specs=[VMEM] * 2,
                out_shape=[pltpu.VMEM((2 + 2 * far, LANES), f32), pltpu.VMEM((4, LANES), f32)],
                scratch_shapes=[pltpu.VMEM((32, LANES), f32)],
                name="pair",
            )(*map(near, args))
            totals = [last]
        back.append(routed(rows[0], blk, step))
        others.append(routed(rows[0], blk, step, cross=True))
    other_total = swapped(totals[0])
    here_total, far_total = pl.pallas_call(
        join_kernel,
        in_specs=[VMEM] * 2,
        out_specs=[VMEM] * 2,
        out_shape=[pltpu.VMEM((2, LANES), f32)] * 2,
        name="join",
    )(near(totals[0]), near(other_total))
    far_total = routed(far_total, blk, (-FAR, -FAR))
    diag, grad, pairs = pl.pallas_call(
        functools.partial(finish_kernel, scale=1.0 / (2.0 * rounds)),
        in_specs=[VMEM] * 6,
        out_specs=[VMEM] * 3,
        out_shape=[
            jax.ShapeDtypeStruct((1, 36), f32),
            jax.ShapeDtypeStruct((1, 6), f32),
            jax.ShapeDtypeStruct((rounds, 36), f32),
        ],
        name="finish",
    )(*(near(x) for x in (*back, *others, here_total, far_total)))
    return diag, grad, pairs.reshape(rounds, 1, 1, 36)


def solution(mesh):
    return jax.shard_map(
        functools.partial(body, blk=mesh.shape["blk"]),
        mesh=mesh,
        in_specs=(
            P("blk", None, None),
            P("blk", None, None),
            P(None, "blk", None, "rep"),
            P(None, "blk", None, "rep", None),
            P(None, "blk", None),
        ),
        out_specs=(P("blk", None), P("blk", None), P(None, "blk", None, None)),
        check_vma=False,
    )
```

```python
import functools

import jax
import jax.numpy as jnp
from jax import lax
from jax.experimental import pallas as pl
from jax.experimental.pallas import tpu as pltpu
from jax.sharding import PartitionSpec as P


NB = 16
BLOCK = 128
LANES = 128
SUBLANES = 8
FAR = 4


VMEM = pl.BlockSpec(memory_space=pltpu.VMEM)
SMEM = pl.BlockSpec(memory_space=pltpu.SMEM)


def routed(block, blk, shifts):
    route = [(i * 2 + r, (i + shifts[r]) % blk * 2 + r) for i in range(blk) for r in range(2)]
    return lax.ppermute(block, ("blk", "rep"), route)


def swapped(block):
    return lax.ppermute(block, "rep", [(0, 1), (1, 0)])


def near(x):
    return pltpu.with_memory_space_constraint(x, pltpu.VMEM)


def pick_lanes(row, lanes):
    return lax.gather(
        row,
        lanes[:, :, None],
        lax.GatherDimensionNumbers(
            offset_dims=(),
            collapsed_slice_dims=(1,),
            start_index_map=(1,),
            operand_batching_dims=(0,),
            start_indices_batching_dims=(0,),
        ),
        slice_sizes=(1, 1),
        mode=lax.GatherScatterMode.PROMISE_IN_BOUNDS,
    )


def step_of(m, rep):
    return 3 - m - 2 * rep


def pack_kernel(src_ref, active_ref, points_ref, normals_ref, index_ref, table_ref, *outs):
    half = lax.axis_index("rep")
    slot = lax.broadcasted_iota(jnp.int32, (SUBLANES, LANES), 0) + half * SUBLANES
    for other, out in enumerate(outs):
        for m in range(2):
            for far in range(2):
                k = step_of(m, 1 - half if other else half) + FAR * far
                for j in range(SUBLANES):
                    b = src_ref[k, j]
                    for c in range(3):
                        out[m, far, c, pl.ds(j, 1), :] = points_ref[c, pl.ds(b, 1), :]
                live = slot < active_ref[0, k]
                out[m, far, 3] = jnp.where(live, index_ref[k], -1).astype(jnp.float32)
    table_ref[0:3] = points_ref[...]
    table_ref[3:6] = normals_ref[...]


def merge_kernel(own_ref, other_ref, *outs):
    for m, out in enumerate(outs):
        for far in range(2):
            for c in range(4):
                out[far, c, pl.ds(0, SUBLANES), :] = own_ref[m, far, c]
                out[far, c, pl.ds(SUBLANES, SUBLANES), :] = other_ref[m, far, c]


def near_kernel(table_ref, message_ref, sums_ref):
    pair_sums(table_ref, message_ref, 0, sums_ref)


def pair_sums(table_ref, message_ref, far, sums_ref):
    shape = (SUBLANES, LANES)
    index = [message_ref[far, 3, pl.ds(h * SUBLANES, SUBLANES), :].astype(jnp.int32) for h in range(2)]
    lanes = [i & (LANES - 1) for i in index]
    high = [i >> 7 for i in index]
    found = [[jnp.zeros(shape, jnp.float32) for _ in range(6)] for _ in range(2)]
    for r in range(table_ref.shape[1]):
        here = [h == r for h in high]
        for c in range(6):
            line = jnp.broadcast_to(table_ref[c, pl.ds(r, 1), :], shape)
            for h in range(2):
                found[h][c] = jnp.where(here[h], pick_lanes(line, lanes[h]), found[h][c])
    parts = []
    for h in range(2):
        p = [message_ref[far, c, pl.ds(h * SUBLANES, SUBLANES), :] for c in range(3)]
        q, n = found[h][:3], found[h][3:]
        resid = n[0] * (p[0] - q[0]) + n[1] * (p[1] - q[1]) + n[2] * (p[2] - q[2])
        weight = 1.0 / (1.0 + resid * resid)
        jacob = [
            p[1] * n[2] - p[2] * n[1],
            p[2] * n[0] - p[0] * n[2],
            p[0] * n[1] - p[1] * n[0],
            n[0],
            n[1],
            n[2],
        ]
        scaled = [weight * x for x in jacob]
        terms = [scaled[a] * jacob[b] for a in range(6) for b in range(a, 6)]
        terms += [scaled[a] * resid for a in range(6)]
        parts.append(terms)
    sums_ref[24:32, :] = jnp.zeros(shape, jnp.float32)
    for t in range(27):
        sums_ref[pl.ds(t, 1), :] = jnp.sum(parts[0][t] + parts[1][t], axis=0, keepdims=True)


def far_kernel(table_ref, message_ref, near_ref, *refs):
    (previous_ref,) = refs[:-3] or (None,)
    rows_ref, totals_ref, sums_s = refs[-3:]
    pair_sums(table_ref, message_ref, 1, sums_s)
    shape = (SUBLANES, LANES)
    row = lax.broadcasted_iota(jnp.int32, shape, 0)
    lane = lax.broadcasted_iota(jnp.int32, shape, 1)
    first, second = lane // 6, lane % 6
    low, top = jnp.minimum(first, second), jnp.maximum(first, second)
    gram_term = jnp.where(lane < 36, low * (11 - low) // 2 + top, -1)
    push_term = jnp.where(lane < 6, 21 + lane, -1)
    scale = 1.0 / (NB * BLOCK)
    for far, sums_ref in enumerate((near_ref, sums_s)):
        gram = jnp.zeros(shape, jnp.float32)
        push = jnp.zeros(shape, jnp.float32)
        for g in range(4):
            column = jnp.sum(sums_ref[pl.ds(SUBLANES * g, SUBLANES), :], axis=1, keepdims=True)
            term = SUBLANES * g + row
            if g < 3:
                gram = jnp.where(gram_term == term, column, gram)
            if g > 1:
                push = jnp.where(push_term == term, column, push)
        gram = jnp.sum(gram, axis=0, keepdims=True) * scale
        push = jnp.sum(push, axis=0, keepdims=True) * scale
        at = 2 * far
        rows_ref[at : at + 1, :] = gram
        rows_ref[at + 1 : at + 2, :] = push
        push = -push
        if previous_ref is not None:
            gram = previous_ref[at : at + 1, :] + gram
            push = previous_ref[at + 1 : at + 2, :] + push
        totals_ref[at : at + 1, :] = gram
        totals_ref[at + 1 : at + 2, :] = push


def split_kernel(totals_ref, here_ref, far_ref):
    here_ref[...] = totals_ref[0:2, :]
    far_ref[...] = totals_ref[2:4, :]


def join_kernel(here_ref, far_ref, total_ref):
    total_ref[...] = here_ref[...] + far_ref[...]


def finish_kernel(*refs, scale):
    rows, totals, (diag_ref, grad_ref, pair_ref) = refs[:4], refs[4:6], refs[6:]
    half = lax.axis_index("rep")
    total = totals[0][...] + totals[1][...]
    for i in range(4):
        m, other = i % 2, i // 2
        for far in range(2):
            k = step_of(m, 1 - half if other else half) + FAR * far
            got = rows[i][2 * far : 2 * far + 2, :]
            pair_ref[pl.ds(k, 1), :] = got[0:1, :36]
            total = total + got
    diag_ref[...] = total[0:1, :36] * scale
    grad_ref[...] = total[1:2, :6] * scale


def body(points, normals, src_block, tgt_index, active, *, blk):
    rounds = src_block.shape[0]
    scan = (3, points.shape[2] // LANES, LANES)
    f32 = jnp.float32
    steps = [tuple(step_of(m, rep) + 1 for rep in range(2)) for m in range(2)]
    table, own, other = pl.pallas_call(
        pack_kernel,
        in_specs=[SMEM, SMEM, VMEM, VMEM, VMEM],
        out_specs=[VMEM] * 3,
        out_shape=[pltpu.VMEM((6, *scan[1:]), f32)] + [pltpu.VMEM((2, 2, 4, SUBLANES, LANES), f32)] * 2,
        name="pack",
    )(
        src_block.reshape(rounds, SUBLANES),
        active.reshape(1, rounds),
        points.reshape(scan),
        normals.reshape(scan),
        tgt_index.reshape(rounds, SUBLANES, BLOCK),
    )
    other = swapped(other)
    far_table = routed(table, blk, (FAR, FAR))
    messages = pl.pallas_call(
        merge_kernel,
        in_specs=[VMEM] * 2,
        out_specs=[VMEM] * 2,
        out_shape=[pltpu.VMEM((2, 4, NB, LANES), f32)] * 2,
        name="merge",
    )(near(own), near(other))
    there = []
    for x, step in zip(messages, steps):
        there.append(routed(x, blk, tuple(-s for s in step)))
    back, totals = [], []
    for message, step in zip(there, steps):
        sums = pl.pallas_call(
            near_kernel,
            in_specs=[VMEM] * 2,
            out_specs=VMEM,
            out_shape=pltpu.VMEM((32, LANES), f32),
            name="near",
        )(near(table), near(message))
        rows, last = pl.pallas_call(
            far_kernel,
            in_specs=[VMEM] * (3 + len(totals)),
            out_specs=[VMEM] * 2,
            out_shape=[pltpu.VMEM((4, LANES), f32)] * 2,
            scratch_shapes=[pltpu.VMEM((32, LANES), f32)],
            name="far",
        )(*map(near, (far_table, message, sums, *totals)))
        totals = [last]
        back.append(routed(rows, blk, step))
    total = pltpu.VMEM((2, LANES), f32)
    here_total, far_total = pl.pallas_call(
        split_kernel, in_specs=[VMEM], out_specs=[VMEM] * 2, out_shape=[total] * 2, name="split"
    )(near(totals[0]))
    far_total = routed(far_total, blk, (-FAR, -FAR))
    total = pl.pallas_call(
        join_kernel, in_specs=[VMEM] * 2, out_specs=VMEM, out_shape=total, name="join"
    )(near(here_total), near(far_total))
    other_total = swapped(total)
    others = []
    for x in back:
        others.append(swapped(x))
    diag, grad, pairs = pl.pallas_call(
        functools.partial(finish_kernel, scale=1.0 / (2.0 * rounds)),
        in_specs=[VMEM] * 6,
        out_specs=[VMEM] * 3,
        out_shape=[
            jax.ShapeDtypeStruct((1, 36), f32),
            jax.ShapeDtypeStruct((1, 6), f32),
            jax.ShapeDtypeStruct((rounds, 36), f32),
        ],
        name="finish",
    )(*(near(x) for x in (*back, *others, total, other_total)))
    return diag, grad, pairs.reshape(rounds, 1, 1, 36)


def solution(mesh):
    return jax.shard_map(
        functools.partial(body, blk=mesh.shape["blk"]),
        mesh=mesh,
        in_specs=(
            P("blk", None, None),
            P("blk", None, None),
            P(None, "blk", None, "rep"),
            P(None, "blk", None, "rep", None),
            P(None, "blk", None),
        ),
        out_specs=(P("blk", None), P("blk", None), P(None, "blk", None, None)),
        check_vma=False,
    )
```

```python
import functools

import jax
import jax.numpy as jnp
from jax import lax
from jax.experimental import pallas as pl
from jax.experimental.pallas import tpu as pltpu
from jax.sharding import PartitionSpec as P


NB = 16
BLOCK = 128
LANES = 128
SUBLANES = 8
FAR = 4


VMEM = pl.BlockSpec(memory_space=pltpu.VMEM)
SMEM = pl.BlockSpec(memory_space=pltpu.SMEM)


def routed(block, blk, shifts, cross=False):
    route = [(i * 2 + r, (i + shifts[r]) % blk * 2 + (1 - r if cross else r)) for i in range(blk) for r in range(2)]
    return lax.ppermute(block, ("blk", "rep"), route)


def swapped(block):
    return lax.ppermute(block, "rep", [(0, 1), (1, 0)])


def near(x):
    return pltpu.with_memory_space_constraint(x, pltpu.VMEM)


def pick_lanes(row, lanes):
    return lax.gather(
        row,
        lanes[:, :, None],
        lax.GatherDimensionNumbers(
            offset_dims=(),
            collapsed_slice_dims=(1,),
            start_index_map=(1,),
            operand_batching_dims=(0,),
            start_indices_batching_dims=(0,),
        ),
        slice_sizes=(1, 1),
        mode=lax.GatherScatterMode.PROMISE_IN_BOUNDS,
    )


def step_of(m, rep):
    return 3 - rep if m else rep


def pack_kernel(src_ref, active_ref, points_ref, normals_ref, index_ref, table_ref, *outs):
    half = lax.axis_index("rep")
    slot = lax.broadcasted_iota(jnp.int32, (SUBLANES, LANES), 0) + half * SUBLANES
    for other, out in enumerate(outs):
        for m in range(2):
            for far in range(2):
                k = step_of(m, 1 - half if other else half) + FAR * far
                for j in range(SUBLANES):
                    b = src_ref[k, j]
                    for c in range(3):
                        out[m, far, c, pl.ds(j, 1), :] = points_ref[c, pl.ds(b, 1), :]
                live = slot < active_ref[0, k]
                out[m, far, 3] = jnp.where(live, index_ref[k], -1).astype(jnp.float32)
    table_ref[0:3] = points_ref[...]
    table_ref[3:6] = normals_ref[...]


def merge_kernel(own_ref, other_ref, *outs):
    for m, out in enumerate(outs):
        for far in range(2):
            for c in range(4):
                out[far, c, pl.ds(0, SUBLANES), :] = own_ref[m, far, c]
                out[far, c, pl.ds(SUBLANES, SUBLANES), :] = other_ref[m, far, c]


def near_kernel(table_ref, message_ref, sums_ref):
    pair_sums(table_ref, message_ref, 0, sums_ref)


def pair_sums(table_ref, message_ref, far, sums_ref):
    shape = (SUBLANES, LANES)
    index = [message_ref[far, 3, pl.ds(h * SUBLANES, SUBLANES), :].astype(jnp.int32) for h in range(2)]
    lanes = [i & (LANES - 1) for i in index]
    high = [i >> 7 for i in index]
    found = [[jnp.zeros(shape, jnp.float32) for _ in range(6)] for _ in range(2)]
    for r in range(table_ref.shape[1]):
        here = [h == r for h in high]
        for c in range(6):
            line = jnp.broadcast_to(table_ref[c, pl.ds(r, 1), :], shape)
            for h in range(2):
                found[h][c] = jnp.where(here[h], pick_lanes(line, lanes[h]), found[h][c])
    parts = []
    for h in range(2):
        p = [message_ref[far, c, pl.ds(h * SUBLANES, SUBLANES), :] for c in range(3)]
        q, n = found[h][:3], found[h][3:]
        resid = n[0] * (p[0] - q[0]) + n[1] * (p[1] - q[1]) + n[2] * (p[2] - q[2])
        weight = 1.0 / (1.0 + resid * resid)
        jacob = [
            p[1] * n[2] - p[2] * n[1],
            p[2] * n[0] - p[0] * n[2],
            p[0] * n[1] - p[1] * n[0],
            n[0],
            n[1],
            n[2],
        ]
        scaled = [weight * x for x in jacob]
        terms = [scaled[a] * jacob[b] for a in range(6) for b in range(a, 6)]
        terms += [scaled[a] * resid for a in range(6)]
        parts.append(terms)
    sums_ref[24:32, :] = jnp.zeros(shape, jnp.float32)
    for t in range(27):
        sums_ref[pl.ds(t, 1), :] = jnp.sum(parts[0][t] + parts[1][t], axis=0, keepdims=True)


def far_kernel(table_ref, message_ref, near_ref, *refs):
    (previous_ref,) = refs[:-3] or (None,)
    rows_ref, totals_ref, sums_s = refs[-3:]
    pair_sums(table_ref, message_ref, 1, sums_s)
    shape = (SUBLANES, LANES)
    row = lax.broadcasted_iota(jnp.int32, shape, 0)
    lane = lax.broadcasted_iota(jnp.int32, shape, 1)
    first, second = lane // 6, lane % 6
    low, top = jnp.minimum(first, second), jnp.maximum(first, second)
    gram_term = jnp.where(lane < 36, low * (11 - low) // 2 + top, -1)
    push_term = jnp.where(lane < 6, 21 + lane, -1)
    scale = 1.0 / (NB * BLOCK)
    for far, sums_ref in enumerate((near_ref, sums_s)):
        gram = jnp.zeros(shape, jnp.float32)
        push = jnp.zeros(shape, jnp.float32)
        for g in range(4):
            column = jnp.sum(sums_ref[pl.ds(SUBLANES * g, SUBLANES), :], axis=1, keepdims=True)
            term = SUBLANES * g + row
            if g < 3:
                gram = jnp.where(gram_term == term, column, gram)
            if g > 1:
                push = jnp.where(push_term == term, column, push)
        gram = jnp.sum(gram, axis=0, keepdims=True) * scale
        push = jnp.sum(push, axis=0, keepdims=True) * scale
        at = 2 * far
        rows_ref[at : at + 1, :] = gram
        rows_ref[at + 1 : at + 2, :] = push
        push = -push
        if previous_ref is not None:
            gram = previous_ref[at : at + 1, :] + gram
            push = previous_ref[at + 1 : at + 2, :] + push
        totals_ref[at : at + 1, :] = gram
        totals_ref[at + 1 : at + 2, :] = push


def split_kernel(totals_ref, here_ref, far_ref):
    here_ref[...] = totals_ref[0:2, :]
    far_ref[...] = totals_ref[2:4, :]


def join_kernel(here_ref, far_ref, total_ref):
    total_ref[...] = here_ref[...] + far_ref[...]


def finish_kernel(*refs, scale):
    rows, totals, (diag_ref, grad_ref, pair_ref) = refs[:4], refs[4:6], refs[6:]
    half = lax.axis_index("rep")
    total = totals[0][...] + totals[1][...]
    for i in range(4):
        m, other = i % 2, i // 2
        for far in range(2):
            k = step_of(m, 1 - half if other else half) + FAR * far
            got = rows[i][2 * far : 2 * far + 2, :]
            pair_ref[pl.ds(k, 1), :] = got[0:1, :36]
            total = total + got
    diag_ref[...] = total[0:1, :36] * scale
    grad_ref[...] = total[1:2, :6] * scale


def body(points, normals, src_block, tgt_index, active, *, blk):
    rounds = src_block.shape[0]
    scan = (3, points.shape[2] // LANES, LANES)
    f32 = jnp.float32
    steps = [tuple(step_of(m, rep) + 1 for rep in range(2)) for m in range(2)]
    table, own, other = pl.pallas_call(
        pack_kernel,
        in_specs=[SMEM, SMEM, VMEM, VMEM, VMEM],
        out_specs=[VMEM] * 3,
        out_shape=[pltpu.VMEM((6, *scan[1:]), f32)] + [pltpu.VMEM((2, 2, 4, SUBLANES, LANES), f32)] * 2,
        name="pack",
    )(
        src_block.reshape(rounds, SUBLANES),
        active.reshape(1, rounds),
        points.reshape(scan),
        normals.reshape(scan),
        tgt_index.reshape(rounds, SUBLANES, BLOCK),
    )
    other = swapped(other)
    far_table = routed(table, blk, (FAR, FAR))
    messages = pl.pallas_call(
        merge_kernel,
        in_specs=[VMEM] * 2,
        out_specs=[VMEM] * 2,
        out_shape=[pltpu.VMEM((2, 4, NB, LANES), f32)] * 2,
        name="merge",
    )(near(own), near(other))
    there = []
    for x, step in zip(messages, steps):
        there.append(routed(x, blk, tuple(-s for s in step)))
    back, totals = [], []
    for message, step in zip(there, steps):
        sums = pl.pallas_call(
            near_kernel,
            in_specs=[VMEM] * 2,
            out_specs=VMEM,
            out_shape=pltpu.VMEM((32, LANES), f32),
            name="near",
        )(near(table), near(message))
        rows, last = pl.pallas_call(
            far_kernel,
            in_specs=[VMEM] * (3 + len(totals)),
            out_specs=[VMEM] * 2,
            out_shape=[pltpu.VMEM((4, LANES), f32)] * 2,
            scratch_shapes=[pltpu.VMEM((32, LANES), f32)],
            name="far",
        )(*map(near, (far_table, message, sums, *totals)))
        totals = [last]
        back.append(routed(rows, blk, step))
    crossed = routed(rows, blk, steps[1], cross=True)
    others = [swapped(back[0]), crossed]
    total = pltpu.VMEM((2, LANES), f32)
    here_total, far_total = pl.pallas_call(
        split_kernel, in_specs=[VMEM], out_specs=[VMEM] * 2, out_shape=[total] * 2, name="split"
    )(near(totals[0]))
    far_total = routed(far_total, blk, (-FAR, -FAR))
    total = pl.pallas_call(
        join_kernel, in_specs=[VMEM] * 2, out_specs=VMEM, out_shape=total, name="join"
    )(near(here_total), near(far_total))
    other_total = swapped(total)
    diag, grad, pairs = pl.pallas_call(
        functools.partial(finish_kernel, scale=1.0 / (2.0 * rounds)),
        in_specs=[VMEM] * 6,
        out_specs=[VMEM] * 3,
        out_shape=[
            jax.ShapeDtypeStruct((1, 36), f32),
            jax.ShapeDtypeStruct((1, 6), f32),
            jax.ShapeDtypeStruct((rounds, 36), f32),
        ],
        name="finish",
    )(*(near(x) for x in (*back, *others, total, other_total)))
    return diag, grad, pairs.reshape(rounds, 1, 1, 36)


def solution(mesh):
    return jax.shard_map(
        functools.partial(body, blk=mesh.shape["blk"]),
        mesh=mesh,
        in_specs=(
            P("blk", None, None),
            P("blk", None, None),
            P(None, "blk", None, "rep"),
            P(None, "blk", None, "rep", None),
            P(None, "blk", None),
        ),
        out_specs=(P("blk", None), P("blk", None), P(None, "blk", None, None)),
        check_vma=False,
    )
```

```python
import functools

import jax
import jax.numpy as jnp
from jax import lax
from jax.experimental import pallas as pl
from jax.experimental.pallas import tpu as pltpu
from jax.sharding import PartitionSpec as P


NB = 16
BLOCK = 128
LANES = 128
SUBLANES = 8
FAR = 4


VMEM = pl.BlockSpec(memory_space=pltpu.VMEM)
SMEM = pl.BlockSpec(memory_space=pltpu.SMEM)


def routed(block, blk, shifts, cross=False):
    route = [(i * 2 + r, (i + shifts[r]) % blk * 2 + (1 - r if cross else r)) for i in range(blk) for r in range(2)]
    return lax.ppermute(block, ("blk", "rep"), route)


def swapped(block):
    return lax.ppermute(block, "rep", [(0, 1), (1, 0)])


def near(x):
    return pltpu.with_memory_space_constraint(x, pltpu.VMEM)


def pick_lanes(row, lanes):
    return lax.gather(
        row,
        lanes[:, :, None],
        lax.GatherDimensionNumbers(
            offset_dims=(),
            collapsed_slice_dims=(1,),
            start_index_map=(1,),
            operand_batching_dims=(0,),
            start_indices_batching_dims=(0,),
        ),
        slice_sizes=(1, 1),
        mode=lax.GatherScatterMode.PROMISE_IN_BOUNDS,
    )


def step_of(m, rep):
    return rep if m else 3 - rep


def pack_kernel(src_ref, active_ref, points_ref, normals_ref, index_ref, table_ref, *outs):
    half = lax.axis_index("rep")
    slot = lax.broadcasted_iota(jnp.int32, (SUBLANES, LANES), 0) + half * SUBLANES
    for other, out in enumerate(outs):
        for m in range(2):
            for far in range(2):
                k = step_of(m, 1 - half if other else half) + FAR * far
                for j in range(SUBLANES):
                    b = src_ref[k, j]
                    for c in range(3):
                        out[m, far, c, pl.ds(j, 1), :] = points_ref[c, pl.ds(b, 1), :]
                live = slot < active_ref[0, k]
                out[m, far, 3] = jnp.where(live, index_ref[k], -1).astype(jnp.float32)
    table_ref[0:3] = points_ref[...]
    table_ref[3:6] = normals_ref[...]


def merge_kernel(own_ref, other_ref, *outs):
    for m, out in enumerate(outs):
        for far in range(2):
            for c in range(4):
                out[far, c, pl.ds(0, SUBLANES), :] = own_ref[m, far, c]
                out[far, c, pl.ds(SUBLANES, SUBLANES), :] = other_ref[m, far, c]


def near_kernel(table_ref, message_ref, sums_ref):
    pair_sums(table_ref, message_ref, 0, sums_ref)


def pair_sums(table_ref, message_ref, far, sums_ref):
    shape = (SUBLANES, LANES)
    index = [message_ref[far, 3, pl.ds(h * SUBLANES, SUBLANES), :].astype(jnp.int32) for h in range(2)]
    lanes = [i & (LANES - 1) for i in index]
    high = [i >> 7 for i in index]
    found = [[jnp.zeros(shape, jnp.float32) for _ in range(6)] for _ in range(2)]
    for r in range(table_ref.shape[1]):
        here = [h == r for h in high]
        for c in range(6):
            line = jnp.broadcast_to(table_ref[c, pl.ds(r, 1), :], shape)
            for h in range(2):
                found[h][c] = jnp.where(here[h], pick_lanes(line, lanes[h]), found[h][c])
    parts = []
    for h in range(2):
        p = [message_ref[far, c, pl.ds(h * SUBLANES, SUBLANES), :] for c in range(3)]
        q, n = found[h][:3], found[h][3:]
        resid = n[0] * (p[0] - q[0]) + n[1] * (p[1] - q[1]) + n[2] * (p[2] - q[2])
        weight = 1.0 / (1.0 + resid * resid)
        jacob = [
            p[1] * n[2] - p[2] * n[1],
            p[2] * n[0] - p[0] * n[2],
            p[0] * n[1] - p[1] * n[0],
            n[0],
            n[1],
            n[2],
        ]
        scaled = [weight * x for x in jacob]
        terms = [scaled[a] * jacob[b] for a in range(6) for b in range(a, 6)]
        terms += [scaled[a] * resid for a in range(6)]
        parts.append(terms)
    sums_ref[24:32, :] = jnp.zeros(shape, jnp.float32)
    for t in range(27):
        sums_ref[pl.ds(t, 1), :] = jnp.sum(parts[0][t] + parts[1][t], axis=0, keepdims=True)


def far_kernel(table_ref, message_ref, near_ref, *refs):
    (previous_ref,) = refs[:-3] or (None,)
    rows_ref, totals_ref, sums_s = refs[-3:]
    pair_sums(table_ref, message_ref, 1, sums_s)
    shape = (SUBLANES, LANES)
    row = lax.broadcasted_iota(jnp.int32, shape, 0)
    lane = lax.broadcasted_iota(jnp.int32, shape, 1)
    first, second = lane // 6, lane % 6
    low, top = jnp.minimum(first, second), jnp.maximum(first, second)
    gram_term = jnp.where(lane < 36, low * (11 - low) // 2 + top, -1)
    push_term = jnp.where(lane < 6, 21 + lane, -1)
    scale = 1.0 / (NB * BLOCK)
    for far, sums_ref in enumerate((near_ref, sums_s)):
        gram = jnp.zeros(shape, jnp.float32)
        push = jnp.zeros(shape, jnp.float32)
        for g in range(4):
            column = jnp.sum(sums_ref[pl.ds(SUBLANES * g, SUBLANES), :], axis=1, keepdims=True)
            term = SUBLANES * g + row
            if g < 3:
                gram = jnp.where(gram_term == term, column, gram)
            if g > 1:
                push = jnp.where(push_term == term, column, push)
        gram = jnp.sum(gram, axis=0, keepdims=True) * scale
        push = jnp.sum(push, axis=0, keepdims=True) * scale
        at = 2 * far
        rows_ref[at : at + 1, :] = gram
        rows_ref[at + 1 : at + 2, :] = push
        push = -push
        if previous_ref is not None:
            gram = previous_ref[at : at + 1, :] + gram
            push = previous_ref[at + 1 : at + 2, :] + push
        totals_ref[at : at + 1, :] = gram
        totals_ref[at + 1 : at + 2, :] = push


def join_kernel(own_ref, other_ref, here_ref, far_ref):
    here_ref[...] = own_ref[0:2, :] + other_ref[0:2, :]
    far_ref[...] = own_ref[2:4, :] + other_ref[2:4, :]


def finish_kernel(*refs, scale):
    rows, totals, (diag_ref, grad_ref, pair_ref) = refs[:4], refs[4:6], refs[6:]
    half = lax.axis_index("rep")
    total = totals[0][...] + totals[1][...]
    for i in range(4):
        m, other = i % 2, i // 2
        for far in range(2):
            k = step_of(m, 1 - half if other else half) + FAR * far
            got = rows[i][2 * far : 2 * far + 2, :]
            pair_ref[pl.ds(k, 1), :] = got[0:1, :36]
            total = total + got
    diag_ref[...] = total[0:1, :36] * scale
    grad_ref[...] = total[1:2, :6] * scale


def body(points, normals, src_block, tgt_index, active, *, blk):
    rounds = src_block.shape[0]
    scan = (3, points.shape[2] // LANES, LANES)
    f32 = jnp.float32
    steps = [tuple(step_of(m, rep) + 1 for rep in range(2)) for m in range(2)]
    table, own, other = pl.pallas_call(
        pack_kernel,
        in_specs=[SMEM, SMEM, VMEM, VMEM, VMEM],
        out_specs=[VMEM] * 3,
        out_shape=[pltpu.VMEM((6, *scan[1:]), f32)] + [pltpu.VMEM((2, 2, 4, SUBLANES, LANES), f32)] * 2,
        name="pack",
    )(
        src_block.reshape(rounds, SUBLANES),
        active.reshape(1, rounds),
        points.reshape(scan),
        normals.reshape(scan),
        tgt_index.reshape(rounds, SUBLANES, BLOCK),
    )
    other = swapped(other)
    far_table = routed(table, blk, (FAR, FAR))
    messages = pl.pallas_call(
        merge_kernel,
        in_specs=[VMEM] * 2,
        out_specs=[VMEM] * 2,
        out_shape=[pltpu.VMEM((2, 4, NB, LANES), f32)] * 2,
        name="merge",
    )(near(own), near(other))
    there = []
    for x, step in zip(messages, steps):
        there.append(routed(x, blk, tuple(-s for s in step)))
    back, totals = [], []
    for message, step in zip(there, steps):
        sums = pl.pallas_call(
            near_kernel,
            in_specs=[VMEM] * 2,
            out_specs=VMEM,
            out_shape=pltpu.VMEM((32, LANES), f32),
            name="near",
        )(near(table), near(message))
        rows, last = pl.pallas_call(
            far_kernel,
            in_specs=[VMEM] * (3 + len(totals)),
            out_specs=[VMEM] * 2,
            out_shape=[pltpu.VMEM((4, LANES), f32)] * 2,
            scratch_shapes=[pltpu.VMEM((32, LANES), f32)],
            name="far",
        )(*map(near, (far_table, message, sums, *totals)))
        totals = [last]
        back.append(routed(rows, blk, step))
    crossed = routed(rows, blk, steps[1], cross=True)
    others = [swapped(back[0]), crossed]
    other_total = swapped(totals[0])
    here_total, far_total = pl.pallas_call(
        join_kernel,
        in_specs=[VMEM] * 2,
        out_specs=[VMEM] * 2,
        out_shape=[pltpu.VMEM((2, LANES), f32)] * 2,
        name="join",
    )(near(totals[0]), near(other_total))
    far_total = routed(far_total, blk, (-FAR, -FAR))
    diag, grad, pairs = pl.pallas_call(
        functools.partial(finish_kernel, scale=1.0 / (2.0 * rounds)),
        in_specs=[VMEM] * 6,
        out_specs=[VMEM] * 3,
        out_shape=[
            jax.ShapeDtypeStruct((1, 36), f32),
            jax.ShapeDtypeStruct((1, 6), f32),
            jax.ShapeDtypeStruct((rounds, 36), f32),
        ],
        name="finish",
    )(*(near(x) for x in (*back, *others, here_total, far_total)))
    return diag, grad, pairs.reshape(rounds, 1, 1, 36)


def solution(mesh):
    return jax.shard_map(
        functools.partial(body, blk=mesh.shape["blk"]),
        mesh=mesh,
        in_specs=(
            P("blk", None, None),
            P("blk", None, None),
            P(None, "blk", None, "rep"),
            P(None, "blk", None, "rep", None),
            P(None, "blk", None),
        ),
        out_specs=(P("blk", None), P("blk", None), P(None, "blk", None, None)),
        check_vma=False,
    )
```

```python
import functools

import jax
import jax.numpy as jnp
from jax import lax
from jax.experimental import pallas as pl
from jax.experimental.pallas import tpu as pltpu
from jax.sharding import PartitionSpec as P


NB = 16
BLOCK = 128
LANES = 128
SUBLANES = 8
FAR = 4


VMEM = pl.BlockSpec(memory_space=pltpu.VMEM)
SMEM = pl.BlockSpec(memory_space=pltpu.SMEM)


def routed(block, blk, shifts, cross=False):
    route = [(i * 2 + r, (i + shifts[r]) % blk * 2 + (1 - r if cross else r)) for i in range(blk) for r in range(2)]
    return lax.ppermute(block, ("blk", "rep"), route)


def swapped(block):
    return lax.ppermute(block, "rep", [(0, 1), (1, 0)])


def near(x):
    return pltpu.with_memory_space_constraint(x, pltpu.VMEM)


def pick_lanes(row, lanes):
    return lax.gather(
        row,
        lanes[:, :, None],
        lax.GatherDimensionNumbers(
            offset_dims=(),
            collapsed_slice_dims=(1,),
            start_index_map=(1,),
            operand_batching_dims=(0,),
            start_indices_batching_dims=(0,),
        ),
        slice_sizes=(1, 1),
        mode=lax.GatherScatterMode.PROMISE_IN_BOUNDS,
    )


def step_of(m, rep):
    return 2 * rep if m else 3 - 2 * rep


def pack_kernel(src_ref, active_ref, points_ref, normals_ref, index_ref, table_ref, *outs):
    half = lax.axis_index("rep")
    slot = lax.broadcasted_iota(jnp.int32, (SUBLANES, LANES), 0) + half * SUBLANES
    for other, out in enumerate(outs):
        for m in range(2):
            for far in range(2):
                k = step_of(m, 1 - half if other else half) + FAR * far
                for j in range(SUBLANES):
                    b = src_ref[k, j]
                    for c in range(3):
                        out[m, far, c, pl.ds(j, 1), :] = points_ref[c, pl.ds(b, 1), :]
                live = slot < active_ref[0, k]
                out[m, far, 3] = jnp.where(live, index_ref[k], -1).astype(jnp.float32)
    table_ref[0:3] = points_ref[...]
    table_ref[3:6] = normals_ref[...]


def merge_kernel(own_ref, other_ref, *outs):
    for m, out in enumerate(outs):
        for far in range(2):
            for c in range(4):
                out[far, c, pl.ds(0, SUBLANES), :] = own_ref[m, far, c]
                out[far, c, pl.ds(SUBLANES, SUBLANES), :] = other_ref[m, far, c]


def near_kernel(table_ref, message_ref, sums_ref):
    pair_sums(table_ref, message_ref, 0, sums_ref)


def pair_sums(table_ref, message_ref, far, sums_ref):
    shape = (SUBLANES, LANES)
    index = [message_ref[far, 3, pl.ds(h * SUBLANES, SUBLANES), :].astype(jnp.int32) for h in range(2)]
    lanes = [i & (LANES - 1) for i in index]
    high = [i >> 7 for i in index]
    found = [[jnp.zeros(shape, jnp.float32) for _ in range(6)] for _ in range(2)]
    for r in range(table_ref.shape[1]):
        here = [h == r for h in high]
        for c in range(6):
            line = jnp.broadcast_to(table_ref[c, pl.ds(r, 1), :], shape)
            for h in range(2):
                found[h][c] = jnp.where(here[h], pick_lanes(line, lanes[h]), found[h][c])
    parts = []
    for h in range(2):
        p = [message_ref[far, c, pl.ds(h * SUBLANES, SUBLANES), :] for c in range(3)]
        q, n = found[h][:3], found[h][3:]
        resid = n[0] * (p[0] - q[0]) + n[1] * (p[1] - q[1]) + n[2] * (p[2] - q[2])
        weight = 1.0 / (1.0 + resid * resid)
        jacob = [
            p[1] * n[2] - p[2] * n[1],
            p[2] * n[0] - p[0] * n[2],
            p[0] * n[1] - p[1] * n[0],
            n[0],
            n[1],
            n[2],
        ]
        scaled = [weight * x for x in jacob]
        terms = [scaled[a] * jacob[b] for a in range(6) for b in range(a, 6)]
        terms += [scaled[a] * resid for a in range(6)]
        parts.append(terms)
    sums_ref[24:32, :] = jnp.zeros(shape, jnp.float32)
    for t in range(27):
        sums_ref[pl.ds(t, 1), :] = jnp.sum(parts[0][t] + parts[1][t], axis=0, keepdims=True)


def far_kernel(table_ref, message_ref, near_ref, *refs):
    (previous_ref,) = refs[:-3] or (None,)
    rows_ref, totals_ref, sums_s = refs[-3:]
    pair_sums(table_ref, message_ref, 1, sums_s)
    shape = (SUBLANES, LANES)
    row = lax.broadcasted_iota(jnp.int32, shape, 0)
    lane = lax.broadcasted_iota(jnp.int32, shape, 1)
    first, second = lane // 6, lane % 6
    low, top = jnp.minimum(first, second), jnp.maximum(first, second)
    gram_term = jnp.where(lane < 36, low * (11 - low) // 2 + top, -1)
    push_term = jnp.where(lane < 6, 21 + lane, -1)
    scale = 1.0 / (NB * BLOCK)
    for far, sums_ref in enumerate((near_ref, sums_s)):
        gram = jnp.zeros(shape, jnp.float32)
        push = jnp.zeros(shape, jnp.float32)
        for g in range(4):
            column = jnp.sum(sums_ref[pl.ds(SUBLANES * g, SUBLANES), :], axis=1, keepdims=True)
            term = SUBLANES * g + row
            if g < 3:
                gram = jnp.where(gram_term == term, column, gram)
            if g > 1:
                push = jnp.where(push_term == term, column, push)
        gram = jnp.sum(gram, axis=0, keepdims=True) * scale
        push = jnp.sum(push, axis=0, keepdims=True) * scale
        at = 2 * far
        rows_ref[at : at + 1, :] = gram
        rows_ref[at + 1 : at + 2, :] = push
        push = -push
        if previous_ref is not None:
            gram = previous_ref[at : at + 1, :] + gram
            push = previous_ref[at + 1 : at + 2, :] + push
        totals_ref[at : at + 1, :] = gram
        totals_ref[at + 1 : at + 2, :] = push


def join_kernel(own_ref, other_ref, here_ref, far_ref):
    here_ref[...] = own_ref[0:2, :] + other_ref[0:2, :]
    far_ref[...] = own_ref[2:4, :] + other_ref[2:4, :]


def finish_kernel(*refs, scale):
    rows, totals, (diag_ref, grad_ref, pair_ref) = refs[:4], refs[4:6], refs[6:]
    half = lax.axis_index("rep")
    total = totals[0][...] + totals[1][...]
    for i in range(4):
        m, other = i % 2, i // 2
        for far in range(2):
            k = step_of(m, 1 - half if other else half) + FAR * far
            got = rows[i][2 * far : 2 * far + 2, :]
            pair_ref[pl.ds(k, 1), :] = got[0:1, :36]
            total = total + got
    diag_ref[...] = total[0:1, :36] * scale
    grad_ref[...] = total[1:2, :6] * scale


def body(points, normals, src_block, tgt_index, active, *, blk):
    rounds = src_block.shape[0]
    scan = (3, points.shape[2] // LANES, LANES)
    f32 = jnp.float32
    steps = [tuple(step_of(m, rep) + 1 for rep in range(2)) for m in range(2)]
    table, own, other = pl.pallas_call(
        pack_kernel,
        in_specs=[SMEM, SMEM, VMEM, VMEM, VMEM],
        out_specs=[VMEM] * 3,
        out_shape=[pltpu.VMEM((6, *scan[1:]), f32)] + [pltpu.VMEM((2, 2, 4, SUBLANES, LANES), f32)] * 2,
        name="pack",
    )(
        src_block.reshape(rounds, SUBLANES),
        active.reshape(1, rounds),
        points.reshape(scan),
        normals.reshape(scan),
        tgt_index.reshape(rounds, SUBLANES, BLOCK),
    )
    other = swapped(other)
    far_table = routed(table, blk, (FAR, FAR))
    messages = pl.pallas_call(
        merge_kernel,
        in_specs=[VMEM] * 2,
        out_specs=[VMEM] * 2,
        out_shape=[pltpu.VMEM((2, 4, NB, LANES), f32)] * 2,
        name="merge",
    )(near(own), near(other))
    there = []
    for x, step in zip(messages, steps):
        there.append(routed(x, blk, tuple(-s for s in step)))
    back, totals = [], []
    for message, step in zip(there, steps):
        sums = pl.pallas_call(
            near_kernel, in_specs=[VMEM] * 2, out_specs=VMEM, out_shape=pltpu.VMEM((32, LANES), f32), name="near"
        )(near(table), near(message))
        rows, last = pl.pallas_call(
            far_kernel,
            in_specs=[VMEM] * (3 + len(totals)),
            out_specs=[VMEM] * 2,
            out_shape=[pltpu.VMEM((4, LANES), f32)] * 2,
            scratch_shapes=[pltpu.VMEM((32, LANES), f32)],
            name="far",
        )(*map(near, (far_table, message, sums, *totals)))
        totals = [last]
        back.append(routed(rows, blk, step))
    crossed = routed(rows, blk, steps[1], cross=True)
    others = [swapped(back[0]), crossed]
    other_total = swapped(totals[0])
    here_total, far_total = pl.pallas_call(
        join_kernel,
        in_specs=[VMEM] * 2,
        out_specs=[VMEM] * 2,
        out_shape=[pltpu.VMEM((2, LANES), f32)] * 2,
        name="join",
    )(near(totals[0]), near(other_total))
    far_total = routed(far_total, blk, (-FAR, -FAR))
    diag, grad, pairs = pl.pallas_call(
        functools.partial(finish_kernel, scale=1.0 / (2.0 * rounds)),
        in_specs=[VMEM] * 6,
        out_specs=[VMEM] * 3,
        out_shape=[
            jax.ShapeDtypeStruct((1, 36), f32),
            jax.ShapeDtypeStruct((1, 6), f32),
            jax.ShapeDtypeStruct((rounds, 36), f32),
        ],
        name="finish",
    )(*(near(x) for x in (*back, *others, here_total, far_total)))
    return diag, grad, pairs.reshape(rounds, 1, 1, 36)


def solution(mesh):
    return jax.shard_map(
        functools.partial(body, blk=mesh.shape["blk"]),
        mesh=mesh,
        in_specs=(
            P("blk", None, None),
            P("blk", None, None),
            P(None, "blk", None, "rep"),
            P(None, "blk", None, "rep", None),
            P(None, "blk", None),
        ),
        out_specs=(P("blk", None), P("blk", None), P(None, "blk", None, None)),
        check_vma=False,
    )
```
